32 devices in a mesh: ep: 8 (over z, y), dp: 4 (over x, core).
Axes of the slice: x: 2, y: 2, z: 4, core: 2. Of those that a mesh axis runs over, the one named last changes fastest.
Arguments:
- tokens: bfloat16 [6144, 2880], P(('ep', 'dp')), may hold values from -64 to 64
- out_grad: bfloat16 [6144, 2880], P(('ep', 'dp')), may hold values from -6 to 6
- indices: int32 [6144, 4], P(('ep', 'dp')), may hold values from 0 to 31, as said below
- expert_rows: bfloat16 [4, 32, 8, 36, 2880], P('dp', 'ep'), may hold values from -0.111328125 to 0.111328125
- router_weight: bfloat16 [2880, 32], replicated, may hold values from -1 to 1
- router_bias: float32 [32], replicated, may hold values from -3 to 3
- balance_scale: float32 [1], replicated, may hold values from 64 to 256
Outputs:
- token_grad: bfloat16 [6144, 2880], P(('ep', 'dp'))
- weight_grad: float32 [2880, 32], P('dp', 'ep')
- balance_loss: float32 [1], replicated
The draws below stay inside these ranges and needn't reach their ends.
Inputs may be any that keep to these rules, and one draw needn't show every extreme that they name: `indices`: each row names 4 different experts. Within the 192 rows of one device no expert is named by more than 36 rows, and some expert is named by exactly 36 rows. Within the rows of one device the 4 experts of one ep index (experts j * 4 to j * 4 + 3) are named by at most 108 rows together, and those of some ep index by exactly 108. Every expert is named by some row of every device.
All inputs are finite; a program needn't handle non-finite values.
Results may differ from the reference program's by a relative error of at most 0.0014.
The reference program's roundings to bfloat16 on the way (of `picked` and `logit_grad`) count: a program that leaves them out, or rounds other values in their place, can miss the bound.
Values may be sent and summed in bfloat16 or wider, within the bound.
A program may use at most 128 MiB of HBM per device.

```python
import math
import jax
import jax.numpy as jnp
from jax import lax

D = 2880
K = 4
EXP_DEV = 4
TOK_DEV = 192
E = 32
CAP = 36
TOKENS = 6144
N_EP = 8
N_DP = 4


def router_table(key):
    sub_key = jax.random.fold_in(key, 11)
    scale = D ** (-0.5)
    return jnp.clip(jax.random.normal(sub_key, (D, E), jnp.float32) * scale, -6.0 * scale, 6.0 * scale)


def draw_router_weight(key, part):
    return router_table(key).astype(jnp.bfloat16)


def block_offsets(key, table_rows):
    pick_key = jax.random.fold_in(key, 29)
    picks = jax.random.randint(pick_key, (N_EP * N_DP, 8), 0, E)
    columns = jnp.take(table_rows.T, picks.reshape(-1), axis=0).reshape(N_EP * N_DP, 8, D)
    per_block = 4.0 * jnp.sum(columns, axis=1)
    return jnp.repeat(per_block, TOK_DEV, axis=0)


def draw_tokens(key, part):
    sub_key = jax.random.fold_in(key, 23)
    table_rows = router_table(key)
    shifted = block_offsets(key, table_rows)
    result = jnp.clip(jax.random.normal(sub_key, (TOKENS, D), jnp.float32), -6.0, 6.0) + shifted
    return jnp.clip(result, -64.0, 64.0).astype(jnp.bfloat16)


def route_block(block_key, common_key):
    key_shift, key_rows, key_cols = jax.random.split(block_key, 3)
    key_heavy, key_inner = jax.random.split(common_key, 2)
    third = CAP // 3
    group_order = jax.random.permutation(key_heavy, N_EP)
    heavy = (group_order % 2 == 0)[:, None]
    shift = jax.random.randint(key_shift, (N_EP, 1), 0, third + 1)
    heavy_loads = jnp.concatenate([jnp.full((N_EP, 2), CAP, jnp.int32), 2 * third - shift, third + shift], axis=1)
    light_loads = jnp.concatenate([jnp.full((N_EP, 1), CAP, jnp.int32), 2 * third - shift, third + shift, jnp.full((N_EP, 1), third, jnp.int32)], axis=1)
    pattern = jnp.where(heavy, heavy_loads, light_loads).astype(jnp.int32)
    inner_scores = jax.random.randint(key_inner, (N_EP, EXP_DEV), 0, 1 << 20) * EXP_DEV + jnp.arange(EXP_DEV, dtype=jnp.int32)[None, :]
    inner_order = jnp.argsort(inner_scores, axis=1)
    loads = jnp.take_along_axis(pattern, inner_order, axis=1).reshape(E)
    bounds = jnp.cumsum(loads)
    positions = jnp.arange(TOK_DEV * K, dtype=jnp.int32)
    labels = jnp.searchsorted(bounds, positions, side='right').astype(jnp.int32)
    grid = labels.reshape(K, TOK_DEV).T
    row_order = jax.random.permutation(key_rows, TOK_DEV)
    grid = jnp.take(grid, row_order, axis=0)
    col_scores = jax.random.randint(key_cols, (TOK_DEV, K), 0, 1 << 20) * K + jnp.arange(K, dtype=jnp.int32)[None, :]
    col_order = jnp.argsort(col_scores, axis=1)
    return jnp.take_along_axis(grid, col_order, axis=1).astype(jnp.int32)


def draw_indices(key, part):
    base_key = jax.random.fold_in(key, 37)
    common_key = jax.random.fold_in(key, 41)
    block_ids = jnp.arange(N_EP * N_DP, dtype=jnp.int32)
    blocks = jax.vmap(lambda block_id: route_block(jax.random.fold_in(base_key, block_id), common_key))(block_ids)
    return blocks.reshape(TOKENS, K).astype(jnp.int32)


def block_levels(key, extent, shards, least, largest):
    factor_of, own = 1.0, jax.random.fold_in(key, 6)
    for position, parts in shards:
        draws = jnp.exp(jax.random.uniform(jax.random.fold_in(own, position), (parts,), jnp.float32, least / len(shards), largest / len(shards)))
        factor_of = factor_of * jnp.repeat(draws, extent[position] // parts).reshape([-1 if axis == position else 1 for axis in range(len(extent))])
    return factor_of


def gaussian(stream_key, extent, scale, bound, pieces=(), kind=jnp.bfloat16):
    entries = jax.random.normal(stream_key, extent, jnp.float32) * scale
    if len(pieces) > 0:
        entries = block_levels(stream_key, extent, pieces, -0.22, 0.18) * entries
    return jnp.clip(entries, min=-bound, max=bound).astype(kind)


def setup_inputs(seed: int = 0) -> dict:
    splits = jax.random.split(jax.random.key(seed), 8)
    return {
        "tokens": draw_tokens(jax.random.fold_in(splits[7], 71), 0),
        "out_grad": gaussian(splits[1], (TOKENS, D), 1.0, 6.0, ((0, 32),)),
        "indices": draw_indices(jax.random.fold_in(splits[7], 71), 0),
        "expert_rows": gaussian(splits[3], (N_DP, E, N_EP, CAP, D), (D ** -0.5), 0.111328125, ((0, 4), (1, 8))),
        "router_weight": draw_router_weight(jax.random.fold_in(splits[7], 71), 0),
        "router_bias": gaussian(splits[5], (E,), 0.5, 3.0, (), jnp.float32),
        "balance_scale": jnp.clip(jnp.exp(jax.random.uniform(splits[6], (1,), jnp.float32, math.log(64.0), math.log(256.0))), 64.0, 256.0),
    }


def reference(tokens, out_grad, indices, expert_rows, router_weight, router_bias, balance_scale):
    logits = jnp.dot(tokens, router_weight, preferred_element_type=jnp.float32) + router_bias
    probability = jax.nn.softmax(logits, axis=-1)
    expert_ids = jnp.arange(E, dtype=jnp.int32)
    onehot = (indices[:, :, None] == expert_ids[None, None, :]).astype(jnp.float32)
    counts = lax.optimization_barrier(jnp.sum(onehot, axis=(0, 1)))
    prob_mean = lax.optimization_barrier(jnp.sum(probability, axis=0)) / TOKENS
    share_of = counts / (TOKENS * K)
    balance_loss = (E * jnp.sum(share_of * prob_mean)).reshape(1)

    def block_dots(block_id):
        ep_index = block_id // N_DP
        dp_index = block_id % N_DP
        cotangent = lax.dynamic_slice_in_dim(out_grad, block_id * TOK_DEV, TOK_DEV, 0)
        chosen_ids = lax.dynamic_slice_in_dim(indices, block_id * TOK_DEV, TOK_DEV, 0)
        group_rows = lax.dynamic_index_in_dim(expert_rows, dp_index, 0, keepdims=False)
        table_rows = lax.dynamic_index_in_dim(group_rows, ep_index, 1, keepdims=False)
        named_by = lax.optimization_barrier(jnp.sum((chosen_ids[:, :, None] == expert_ids[None, None, :]).astype(jnp.int32), axis=1))
        before = jnp.cumsum(named_by, axis=0) - named_by
        slot_index = jnp.take_along_axis(before, chosen_ids, axis=1)
        row_index = (chosen_ids * CAP + slot_index).astype(jnp.int32)
        picked = table_rows.reshape(E * CAP, D)[row_index]
        return jnp.einsum('td,tkd->tk', cotangent.astype(jnp.float32), picked.astype(jnp.float32))
    pair_dots = lax.map(block_dots, jnp.arange(N_EP * N_DP, dtype=jnp.int32)).reshape(TOKENS, K)
    chosen_logits = jnp.take_along_axis(logits, indices, axis=1)
    mix_weight = jax.nn.softmax(chosen_logits, axis=-1)
    sel_grad = mix_weight * (pair_dots - lax.optimization_barrier(jnp.sum(mix_weight * pair_dots, axis=1, keepdims=True)))
    balance_push = balance_scale[0] * E * share_of
    spread = probability * (balance_push[None, :] - lax.optimization_barrier(jnp.sum(probability * balance_push[None, :], axis=1, keepdims=True)))
    logit_grad = (spread + lax.optimization_barrier(jnp.sum(onehot * sel_grad[:, :, None], axis=1))).astype(jnp.bfloat16)
    token_grad = jnp.dot(logit_grad, router_weight.T, preferred_element_type=jnp.float32).astype(jnp.bfloat16)
    weight_grad = jnp.dot(tokens.T, logit_grad, preferred_element_type=jnp.float32) / math.sqrt(TOKENS)
    return (token_grad, weight_grad, balance_loss)
```

```python
import functools
import math

import jax
import jax.numpy as jnp
from jax import lax
from jax.experimental import pallas as pl
from jax.experimental.pallas import tpu as pltpu
from jax.sharding import PartitionSpec as P

MESH = pl.DeviceIdType.MESH
F32 = jnp.float32
BF16 = jnp.bfloat16
CHUNK = 768
LAG = 4


def dot_nt(x, y, precision=None):
    return lax.dot_general(
        x, y, (((1,), (1,)), ((), ())), preferred_element_type=F32, precision=precision
    )


def dot_nn(x, y, precision=None):
    return lax.dot_general(
        x, y, (((1,), (0,)), ((), ())), preferred_element_type=F32, precision=precision
    )


def kernel(cfg, *refs):
    (ep, dp, tok_dev, chosen, experts, exp_dev, cap, packed, widths, starts, swapped, late, token_total) = cfg
    line = ep // 2
    last = line - 1
    chunks = len(widths)
    every = range(chunks)
    kept = [c for c in every if c not in swapped]
    (idx_in, grad_in, rows_in, tok_in, wt_in, bias_in, scale_in, tg_out, wg_out, loss_out) = refs[:10]
    refs = refs[10:]
    hop = refs[5 * chunks:6 * chunks]
    hop_n = refs[6 * chunks:7 * chunks]
    back_n = refs[7 * chunks:8 * chunks]
    xb = refs[:chunks]
    lsend = refs[chunks:2 * chunks]
    lrecv = refs[2 * chunks:3 * chunks]
    rows_v = refs[3 * chunks:4 * chunks]
    back = refs[4 * chunks:5 * chunks]
    (tok_v, wt_v, bias_v, scale_v, s_in, loss_v, wg_v, s_out,
     rows_raw, piled, tgt_r, acc_r, rst_r, rbuf_r, s_back, r_back, r_hop, s_near, r_hop_n, r_back_n, s_rr, r_rr, tgt_n, acc_n, tg_v,
     idx_all, pin, pout, tgt_x, tgt_p, acc_x, acc_p, rst, rbuf, tks, tkr, logit_v, prob_v,
     named_v, st_dp, st_m, st_z, lgd, ws, wr,
     s_rows, s_own, s_idx, r_idx, s_right, s_left, r_x, s_leaf, r_leaf, s_rep, r_rep,
     s_tk, r_tk, s_sd, r_sd, s_st, r_st, s_lg, r_lg, s_w, r_w) = refs[8 * chunks:]
    me = lax.axis_index("ep")
    md = lax.axis_index("dp")
    pos = me // 2
    side = lax.rem(me, 2)
    mate = pos * 2 + 1 - side
    at_end = jnp.logical_or(pos == 0, pos == last)
    near_end = jnp.logical_or(pos == 1, pos == last - 1)
    end = jnp.where(pos * 2 < line, 0, last)
    near = jnp.where(pos * 2 < line, 1, last - 1)
    far = last - end

    def ep_id(other):
        return (other, md)

    def remote(src, dst, s, r, dev):
        return pltpu.make_async_remote_copy(
            src_ref=src, dst_ref=dst, send_sem=s, recv_sem=r, device_id=dev, device_id_type=MESH
        )

    def ep_peer(s):
        return lax.rem(me + s, ep)

    def dp_peer(s):
        return lax.rem(md + s, dp)

    barrier = pltpu.get_barrier_semaphore()

    def greet(dev):
        pl.semaphore_signal(barrier, inc=1, device_id=dev, device_id_type=MESH)

    @pl.when(pos < last)
    def _():
        greet(ep_id(me + 2))

    @pl.when(pos > 0)
    def _():
        greet(ep_id(me - 2))

    greet(ep_id(mate))
    for s in range(1, dp):
        greet((me, dp_peer(s)))

    idx_here = pltpu.make_async_copy(idx_in, idx_all.at[me], s_in.at[0])
    own = [
        pltpu.make_async_copy(grad_in.at[:, pl.ds(starts[c], widths[c])], xb[c].at[pos], s_own.at[c])
        for c in every
    ]
    rows_copy = pltpu.make_async_copy(rows_in, rows_raw, s_rows)
    small = [
        pltpu.make_async_copy(tok_in, tok_v, s_in.at[1]),
        pltpu.make_async_copy(wt_in, wt_v, s_in.at[2]),
        pltpu.make_async_copy(bias_in, bias_v, s_in.at[3]),
        pltpu.make_async_copy(scale_in, scale_v, s_in.at[4]),
    ]
    idx_here.start()
    for copy in own:
        copy.start()
    rows_copy.start()
    for copy in small:
        copy.start()
    pl.semaphore_wait(
        barrier, dp + (pos < last).astype(jnp.int32) + (pos > 0).astype(jnp.int32)
    )

    def idx_copy(q, way, dev):
        at = q * 2 + side
        return remote(idx_all.at[at], idx_all.at[at], s_idx.at[way], r_idx.at[at], ep_id(dev))

    def idx_right(q):
        return idx_copy(q, 0, me + 2)

    def idx_left(q):
        return idx_copy(q, 1, me - 2)

    def idx_mate(q):
        return idx_copy(q, 2, mate)

    def idx_from_mate(q):
        at = q * 2 + 1 - side
        return remote(idx_all.at[at], idx_all.at[at], s_idx.at[2], r_idx.at[at], ep_id(mate))

    def loop_ep(fn):
        def body(s, carry):
            fn(s)
            return carry
        lax.fori_loop(1, ep, body, 0)

    def to_right(q, c):
        return remote(xb[c].at[q], xb[c].at[q], s_right.at[c], r_x.at[q, c], ep_id(me + 2))

    def to_left(q, c):
        return remote(xb[c].at[q], xb[c].at[q], s_left.at[c], r_x.at[q, c], ep_id(me - 2))

    def leaf(q, c):
        return remote(lsend[c].at[q], lrecv[c].at[q], s_leaf.at[c], r_leaf.at[q, c], ep_id(mate))

    def hop_rows(c):
        return remote(rows_v[c].at[far * 2 + 1 - side], hop[c], s_back.at[c], r_hop.at[c], ep_id(mate))

    def send_back(b, c):
        src = rows_v[c].at[far * 2 + side] if b == 0 else hop[c]
        at = side if b == 0 else 1 - side
        return remote(src, back[c].at[at], s_back.at[c], r_back.at[c], ep_id(near * 2 + side))

    def back_arrival(c):
        return remote(back[c], back[c], s_back.at[c], r_back.at[c], ep_id(end * 2 + side))

    def hop_near(c):
        return remote(rows_v[c].at[near * 2 + 1 - side], hop_n[c], s_near.at[c], r_hop_n.at[c], ep_id(mate))

    def send_near(c):
        return remote(hop_n[c], back_n[c], s_near.at[c], r_back_n.at[c], ep_id(near * 2 + side))

    def near_arrival(c):
        return remote(back_n[c], back_n[c], s_near.at[c], r_back_n.at[c], ep_id(end * 2 + side))

    def back_reply():
        return remote(rst_r, rbuf_r, s_rr, r_rr, ep_id(far * 2 + side))

    def back_reply_arrival():
        return remote(rst_r, rbuf_r, s_rr, r_rr, ep_id((last - near) * 2 + side))

    def reply(j):
        return remote(rst.at[j], rbuf.at[me], s_rep, r_rep, ep_id(j))

    def st_copy(q, way, dev):
        return remote(st_z.at[q], st_z.at[q], s_st.at[way], r_st.at[q], ep_id(dev))

    def st_right(q):
        return st_copy(q, 0, me + 2)

    def st_left(q):
        return st_copy(q, 1, me - 2)

    def st_mate(at):
        return remote(st_m.at[at], st_m.at[at], s_st.at[2], r_st.at[line], ep_id(mate))

    for copy in own:
        copy.wait()
    idx_here.wait()

    @pl.when(pos < last)
    def _():
        idx_right(pos).start()

    @pl.when(pos > 0)
    def _():
        idx_left(pos).start()

    idx_mate(pos).start()
    for c in every:
        @pl.when(pos < last - (c in late))
        def _():
            to_right(pos, c).start()

        @pl.when(pos > 0 + (c in late))
        def _():
            to_left(pos, c).start()

    expert_row = lax.broadcasted_iota(jnp.int32, (experts, tok_dev), 0)
    eye_r = lax.broadcasted_iota(jnp.int32, (experts, experts), 0)
    eye_c = lax.broadcasted_iota(jnp.int32, (experts, experts), 1)
    t_from = lax.broadcasted_iota(jnp.int32, (tok_dev, tok_dev), 0)
    t_to = lax.broadcasted_iota(jnp.int32, (tok_dev, tok_dev), 1)
    upper = jnp.where(t_from < t_to, 1.0, 0.0).astype(BF16)
    row8 = lax.broadcasted_iota(jnp.int32, (8, tok_dev), 0)
    slot_p = lax.broadcasted_iota(jnp.int32, (packed, tok_dev), 0).astype(F32)

    def upright(line_of):
        return jnp.sum(jnp.where(eye_r == eye_c, line_of, 0.0), axis=1, keepdims=True)

    def plan(table, group):
        who = jnp.where(row8 < exp_dev, group * exp_dev + row8, -2)
        hit = jnp.zeros((8, tok_dev), F32)
        for k in range(chosen):
            hit = hit + jnp.where(table[k:k + 1, :] == who, 1.0, 0.0)
        need = jnp.max(hit, axis=0, keepdims=True)
        stack = jnp.where(row8 == exp_dev, need, hit)
        before = dot_nn(stack.astype(BF16), upper)
        place = jnp.where(need > 0.5, before[exp_dev:exp_dev + 1, :], -1.0)
        target = jnp.where(hit > 0.5, before, -1.0)
        pack = jnp.where(slot_p == place, 1.0, 0.0).astype(BF16)
        return target, pack

    def plan_block(q):
        table = idx_all[q * 2 + side]
        _, pack = plan(table, mate)
        pout[q] = pack
        target, _ = plan(table, me)
        tgt_x[q] = target
        acc_x[q] = jnp.zeros((8, tok_dev), F32)

    def plan_leaf(q):
        target, pack = plan(idx_all[q * 2 + 1 - side], me)
        pin[q] = pack
        tgt_p[q] = dot_nt((target + 1.0).astype(BF16), pack) - 1.0
        acc_p[q] = jnp.zeros((8, packed), F32)

    def plan_back():
        for b in range(2):
            tgt_r[b], _ = plan(idx_all[far * 2 + side], end * 2 + b)
            acc_r[b] = jnp.zeros((8, tok_dev), F32)
        tgt_n[...], _ = plan(idx_all[me], end * 2 + 1 - side)
        acc_n[...] = jnp.zeros((8, tok_dev), F32)

    deep = piled.shape[1] // ep
    slot_r = lax.broadcasted_iota(jnp.int32, (deep, cap * ep), 0)
    lies = lax.broadcasted_iota(jnp.int32, (deep, cap * ep), 1)
    spare = rows_v[0].shape[1] - exp_dev * cap

    def sort_rows(c):
        w = widths[c]
        order = jnp.concatenate(
            [jnp.where(jnp.logical_and(lies == slot_r * ep + j, slot_r < cap), 1.0, 0.0) for j in range(ep)], axis=0
        ).astype(BF16)
        for e in range(exp_dev):
            piled[e, :, 0:w] = dot_nn(order, rows_raw[e, :, starts[c]:starts[c] + w])

        def put(j, carry):
            at = pl.ds(pl.multiple_of(j * deep, 8), deep)
            pieces = [piled[e, at, 0:w][0:cap, :] for e in range(exp_dev)]
            if spare:
                pieces.append(jnp.zeros((spare, w), F32))
            rows_v[c][j] = jnp.concatenate(pieces, axis=0).astype(BF16)
            return carry

        lax.fori_loop(0, ep, put, 0)

    def gathered(table, block, target, count):
        height = table.shape[0]
        slot = lax.broadcasted_iota(jnp.int32, (height, count), 0).astype(F32)
        row = lax.broadcasted_iota(jnp.int32, (8, count), 0)
        dots = dot_nt(table, block)
        out = jnp.zeros((8, count), F32)
        for e in range(exp_dev):
            want = jnp.where(target[e:e + 1, :] >= 0.0, target[e:e + 1, :] + e * cap, -1.0)
            one = jnp.sum(jnp.where(slot == want, dots, 0.0), axis=0, keepdims=True)
            out = jnp.where(row == e, one, out)
        return out

    def give_leaf(q, c):
        lsend[c][q] = dot_nn(pout[q], xb[c][q]).astype(BF16)
        leaf(q, c).start()

    def use_block(q, c):
        acc_x[q] += gathered(rows_v[c][q * 2 + side], xb[c][q], tgt_x[q], tok_dev)

    def use_leaf(q, c):
        leaf(q, c).wait_recv()
        acc_p[q] += gathered(rows_v[c][q * 2 + 1 - side], lrecv[c][q], tgt_p[q], packed)

    def answer(j, value):
        rst[j] = value
        reply(j).start()

    def done_block(q):
        answer(q * 2 + side, acc_x[q])

    def done_leaf(q):
        answer(q * 2 + 1 - side, dot_nn(acc_p[q], pin[q].astype(F32), lax.Precision.HIGHEST))

    def meets(s, c, tail):
        left, right = pos - s >= 0, pos + s < line
        if s == last and c in swapped:
            return ()
        if s == 1 and c in late:
            inner = at_end if tail else jnp.logical_not(at_end)
            left, right = jnp.logical_and(left, inner), jnp.logical_and(right, inner)
        return ((pos - s, left, True), (pos + s, right, False))

    def closes(s, c, tail, finish, q):
        if s == 1 and len(late) and finish is done_block:
            if tail:
                if c == late[-1]:
                    finish(q)
            elif c == chunks - 1:
                @pl.when(jnp.logical_not(at_end))
                def _():
                    finish(q)
        elif c == (kept[-1] if s == last else chunks - 1):
            finish(q)

    def learn(s):
        for q, ok, rightward in ((pos - s, pos - s >= 0, True), (pos + s, pos + s < line, False)):
            @pl.when(ok)
            def _(q=q, rightward=rightward):
                step = idx_right if rightward else idx_left
                step(q).wait_recv()

                @pl.when(pos < last if rightward else pos > 0)
                def _():
                    step(q).start()
                    if s == last - 1 and len(swapped):
                        plan_back()

                idx_mate(q).start()
                plan_block(q)

    def learn_leaf(s):
        for q, ok in ((pos - s, pos - s >= 0), (pos + s, pos + s < line))[:1 if s == 0 else 2]:
            @pl.when(ok)
            def _(q=q):
                idx_from_mate(q).wait_recv()
                plan_leaf(q)

    def arrive(s, c, tail=False):
        for q, ok, rightward in meets(s, c, tail):
            @pl.when(ok)
            def _(q=q, rightward=rightward):
                step = to_right if rightward else to_left
                step(q, c).wait_recv()

                @pl.when(pos < last if rightward else pos > 0)
                def _():
                    if not (s == last - 1 and c in swapped):
                        step(q, c).start()
                    if s == last - 1 and c == kept[-1]:
                        for n in late:
                            step(pos, n).start()

                if not tail:
                    give_leaf(q, c)

    def use(s, c, tail=False):
        for q, ok, rightward in meets(s, c, tail):
            @pl.when(ok)
            def _(q=q, rightward=rightward):
                use_block(q, c)
                closes(s, c, tail, done_block, q)
                if s == last - 1 and c in swapped:
                    @pl.when(pos < last if rightward else pos > 0)
                    def _():
                        back_arrival(c).wait_recv()
                        for b in range(2):
                            acc_r[b] += gathered(back[c][b], xb[c][q], tgt_r[b], tok_dev)
                        if c == swapped[-1]:
                            rst_r[...] = acc_r[...]
                            back_reply().start()
                            for n in late:
                                near_arrival(n).wait_recv()
                                acc_n[...] += gathered(back_n[n][...], xb[n][pos], tgt_n[...], tok_dev)

    def take(s, c):
        if s == 0:
            use_leaf(pos, c)
            if c == chunks - 1:
                done_leaf(pos)
            return
        for q, ok, _ in meets(s, c, False):
            @pl.when(ok)
            def _(q=q):
                use_leaf(q, c)
                closes(s, c, False, done_leaf, q)

    def settle(s, c):
        if c == 0:
            learn_leaf(s)
        take(s, c)

    def pass_rows(c):
        @pl.when(at_end)
        def _():
            if c in swapped:
                hop_rows(c).wait_recv()
                send_back(1, c).start()
            if c in late:
                hop_near(c).wait_recv()
                send_near(c).start()

    def sort_step(c):
        sort_rows(c)
        if c in swapped or c in late:
            @pl.when(at_end)
            def _():
                if c in swapped:
                    hop_rows(c).start()
                    send_back(0, c).start()
                if c in late:
                    hop_near(c).start()
        use_block(pos, c)
        if c == chunks - 1:
            rbuf[me] = acc_x[pos]

    part = tok_in.shape[1] // dp

    def tk_copy(s):
        return remote(tks.at[dp_peer(s)], tkr.at[md], s_tk, r_tk, (me, dp_peer(s)))

    def tk_all():
        return remote(tks.at[pl.ds(0, dp - 1)], tkr.at[pl.ds(0, dp - 1)], s_tk, r_tk, (me, dp_peer(1)))

    def sd_copy(s):
        return remote(st_dp.at[md], st_dp.at[md], s_sd, r_sd, (me, dp_peer(s)))

    def sd_all():
        return remote(st_dp.at[pl.ds(0, dp - 1)], st_dp.at[pl.ds(0, dp - 1)], s_sd, r_sd, (me, dp_peer(1)))

    def route():
        for copy in small:
            copy.wait()
        idx = idx_all[me]
        named = jnp.zeros((experts, tok_dev), F32)
        for k in range(chosen):
            named = named + jnp.where(idx[k:k + 1, :] == expert_row, 1.0, 0.0)
        logits = dot_nt(wt_v[...], tok_v[...]) + upright(bias_v[...])
        top = jnp.max(logits, axis=0, keepdims=True)
        power = jnp.exp(logits - top)
        prob = power / jnp.sum(power, axis=0, keepdims=True)
        logit_v[...] = logits
        prob_v[...] = prob
        named_v[...] = named
        ones = jnp.ones((8, tok_dev), F32)
        count_row = dot_nt(ones, named, lax.Precision.HIGHEST)
        prob_row = dot_nt(ones, prob, lax.Precision.HIGHEST)
        stat_row = lax.broadcasted_iota(jnp.int32, (8, experts), 0)
        st_dp[md] = jnp.where(stat_row == 0, count_row, prob_row)
        for s in range(1, dp):
            sd_copy(s).start()

    def share_tokens():
        for d in range(dp):
            tks[d] = tok_v[:, d * part:(d + 1) * part]
        for s in range(1, dp):
            tk_copy(s).start()
        tkr[md] = tks[md]

    def pair_stats():
        sd_all().wait_recv()
        total = st_dp[0]
        for d in range(1, dp):
            total = total + st_dp[d]
        st_m[side] = total
        st_mate(side).start()

    def share_stats():
        st_mate(1 - side).wait_recv()
        st_z[pos] = st_m[0] + st_m[1]

        @pl.when(pos < last)
        def _():
            st_right(pos).start()

        @pl.when(pos > 0)
        def _():
            st_left(pos).start()

    def pass_stats(s):
        for q, ok, rightward in ((pos - s, pos - s >= 0, True), (pos + s, pos + s < line, False)):
            @pl.when(ok)
            def _(q=q, rightward=rightward):
                step = st_right if rightward else st_left
                step(q).wait_recv()

                @pl.when(pos < last if rightward else pos > 0)
                def _():
                    step(q).start()

    plan_block(pos)
    for c in every:
        give_leaf(pos, c)
    rows_copy.wait()
    for c in every:
        if c == max(chunks - 2, 0):
            learn(1)
            arrive(1, 0)
        sort_step(c)
    steps = [(0, c) for c in every] + [(s, c) for s in range(1, line) for c in every]
    taken = 0
    for n, (s, c) in enumerate(steps):
        if s > 0:
            if c == 0:
                if s > 1:
                    learn(s)
            if (s, c) != (1, 0):
                arrive(s, c)
            use(s, c)
            if s == 2 and (c in swapped or c in late):
                pass_rows(c)
            if s == 2 and c == chunks - 1:
                pass_stats(1)
            if (s, c) == (1, 1 if chunks > 1 else 0):
                route()
                share_tokens()
            if (s, c) == (1, max(chunks - 2, 0)):
                pair_stats()
            if (s, c) == ((2, 0) if last > 1 else (1, chunks - 1)):
                share_stats()
            while taken <= n - LAG:
                settle(*steps[taken])
                taken += 1
    for c in late:
        arrive(1, c, True)
        use(1, c, True)
    for step in steps[taken:]:
        settle(*step)
    for s in range(2 if last > 1 else 1, line):
        pass_stats(s)
    stats = st_z[0]
    for q in range(1, line):
        stats = stats + st_z[q]
    share = stats[0:1, :] / (token_total * chosen)
    mean = stats[1:2, :] / token_total
    loss_v[...] = experts * jnp.sum(share * mean, axis=1, keepdims=True)
    loss_copy = pltpu.make_async_copy(loss_v, loss_out, s_out.at[0])
    loss_copy.start()
    push_row = scale_v[...] * experts * share
    push = upright(push_row)
    prob = prob_v[...]
    spread = prob * (push - jnp.sum(prob * push, axis=0, keepdims=True))
    named = named_v[...]
    logits = logit_v[...]
    high = jnp.max(jnp.where(named > 0.5, logits, -jnp.inf), axis=0, keepdims=True)
    mix = jnp.where(named > 0.5, jnp.exp(jnp.minimum(logits - high, 0.0)), 0.0)
    mix = mix / jnp.sum(mix, axis=0, keepdims=True)

    remote(rst.at[pl.ds(0, ep - 1)], rbuf.at[pl.ds(0, ep - 1)], s_rep, r_rep, ep_id(mate)).wait_recv()
    if len(swapped):
        @pl.when(at_end)
        def _():
            back_reply_arrival().wait_recv()
            for b in range(2):
                rbuf[far * 2 + b] += rbuf_r[b]

        @pl.when(near_end)
        def _():
            rbuf[end * 2 + 1 - side] += acc_n[...]
    dots = jnp.concatenate([rbuf[j, 0:exp_dev, :] for j in range(ep)], axis=0)
    sel = mix * (dots - jnp.sum(mix * dots, axis=0, keepdims=True))
    grad = (spread + sel).astype(BF16)
    lgd[md] = grad

    def lg_copy(s):
        return remote(lgd.at[md], lgd.at[md], s_lg, r_lg, (me, dp_peer(s)))

    def lg_all():
        return remote(lgd.at[pl.ds(0, dp - 1)], lgd.at[pl.ds(0, dp - 1)], s_lg, r_lg, (me, dp_peer(1)))

    for s in range(1, dp):
        lg_copy(s).start()
    for c in every:
        at = slice(starts[c], starts[c] + widths[c])
        tg_v[:, at] = lax.dot_general(
            grad, wt_v[:, at], (((0,), (0,)), ((), ())), preferred_element_type=F32
        ).astype(BF16)
    tg_store = pltpu.make_async_copy(tg_v, tg_out, s_out.at[1])
    tg_store.start()
    tk_all().wait_recv()
    lg_all().wait_recv()
    term = dot_nn(lgd[0], tkr[0])
    for d in range(1, dp):
        term = term + dot_nn(lgd[d], tkr[d])
    for j in range(ep):
        ws[j] = term[j * exp_dev:(j + 1) * exp_dev, :]
    wr[me] = ws[me]

    def w_copy(s_):
        return remote(ws.at[ep_peer(s_)], wr.at[me], s_w, r_w, ep_id(ep_peer(s_)))

    def w_all():
        return remote(ws.at[pl.ds(0, ep - 1)], wr.at[pl.ds(0, ep - 1)], s_w, r_w, ep_id(mate))

    loop_ep(lambda s_: w_copy(s_).start())

    def sent(ref, sem, count):
        for n in range(1, line + 1):
            @pl.when(count == n)
            def _(n=n):
                piece = ref.at[pl.ds(0, n)]
                remote(piece, piece, sem, sem, ep_id(mate)).wait_send()

    ups = jnp.where(pos < last, pos + 1, 0)
    downs = jnp.where(pos > 0, line - pos, 0)
    for buf, sem in ((idx_all, s_idx), (st_z, s_st)):
        sent(buf, sem.at[0], ups)
        sent(buf, sem.at[1], downs)
    sent(idx_all, s_idx.at[2], line)
    st_mate(side).wait_send()
    for c in every:
        short = 1 if c in swapped else 0
        sent(xb[c], s_right.at[c], ups - jnp.where(pos == last - 1, short, 0))
        sent(xb[c], s_left.at[c], downs - jnp.where(pos == 1, short, 0))
        skipped = short + (1 if c in late else 0)
        sent(lsend[c], s_leaf.at[c], line - jnp.where(at_end, skipped, 0))
    if len(swapped):
        @pl.when(at_end)
        def _():
            for c in swapped:
                piece = rows_v[c].at[pl.ds(0, 3)]
                remote(piece, piece, s_back.at[c], s_back.at[c], ep_id(mate)).wait_send()
            for c in late:
                piece = rows_v[c].at[pl.ds(0, 2)]
                remote(piece, piece, s_near.at[c], s_near.at[c], ep_id(mate)).wait_send()

        @pl.when(near_end)
        def _():
            back_reply().wait_send()
    remote(rst.at[pl.ds(0, ep - 1)], rbuf.at[pl.ds(0, ep - 1)], s_rep, r_rep, ep_id(mate)).wait_send()
    sd_all().wait_send()
    tk_all().wait_send()
    lg_all().wait_send()
    loss_copy.wait()
    tg_store.wait()
    w_all().wait_recv()
    out = lax.fori_loop(1, ep, lambda j, acc: acc + wr[j], wr[0])
    wg_v[...] = out / math.sqrt(token_total)
    wg_copy = pltpu.make_async_copy(wg_v, wg_out, s_out.at[2])
    wg_copy.start()
    w_all().wait_send()
    wg_copy.wait()


def cut(width):
    if width <= 3 * CHUNK + CHUNK // 2 or width > 4 * CHUNK:
        widths = tuple(min(CHUNK, width - s) for s in range(0, width, CHUNK))
        return widths, tuple(sum(widths[:c]) for c in range(len(widths))), (), ()
    half = CHUNK // 2
    rest = width - 3 * CHUNK - half
    return (CHUNK, rest, half, CHUNK, CHUNK), (0, width - rest, CHUNK, CHUNK + half, 2 * CHUNK + half), (2, 3, 4), (2, 1)


def on_device(tokens, out_grad, indices, expert_rows, router_weight, router_bias, balance_scale):
    tok_dev, width = tokens.shape
    chosen = indices.shape[1]
    experts = router_weight.shape[1]
    exp_dev, cap = expert_rows.shape[1], expert_rows.shape[3]
    ep = lax.axis_size("ep")
    dp = lax.axis_size("dp")
    line = ep // 2
    packed = -(-min(tok_dev, (exp_dev - 1) * cap) // 16) * 16
    widths, starts, swapped, late = cut(width)
    chunks = len(widths)
    if line < 4:
        swapped, late = (), ()
    cfg = (ep, dp, tok_dev, chosen, experts, exp_dev, cap, packed, widths, starts, swapped, late, tok_dev * ep * dp)
    part = width // dp
    rows_t = jnp.transpose(expert_rows[0], (0, 2, 1, 3)).reshape(exp_dev, cap * ep, width)
    hbm = pl.BlockSpec(memory_space=pl.ANY)
    dma = pltpu.SemaphoreType.DMA
    scratch = [pltpu.VMEM((line, tok_dev, w), BF16) for w in widths]
    scratch += [pltpu.VMEM((line, packed, w), BF16) for w in widths]
    scratch += [pltpu.VMEM((line, packed, w), BF16) for w in widths]
    scratch += [pltpu.VMEM((ep, -(-exp_dev * cap // 16) * 16, w), BF16) for w in widths]
    scratch += [pltpu.VMEM((2, -(-exp_dev * cap // 16) * 16, w), BF16) for w in widths]
    scratch += [pltpu.VMEM((-(-exp_dev * cap // 16) * 16, w), BF16) for w in widths]
    scratch += [pltpu.VMEM((-(-exp_dev * cap // 16) * 16, w), BF16) for w in widths]
    scratch += [pltpu.VMEM((-(-exp_dev * cap // 16) * 16, w), BF16) for w in widths]
    scratch += [
        pltpu.VMEM((tok_dev, width), BF16),
        pltpu.VMEM((experts, width), BF16),
        pltpu.VMEM((1, experts), F32),
        pltpu.VMEM((1, 1), F32),
        dma((5,)),
        pltpu.VMEM((1, 1), F32),
        pltpu.VMEM((exp_dev, part), F32),
        dma((3,)),
        pltpu.VMEM((exp_dev, cap * ep, width), BF16),
        pltpu.VMEM((exp_dev, ep * (-(-cap // 8) * 8), max(widths)), F32),
        pltpu.VMEM((2, 8, tok_dev), F32),
        pltpu.VMEM((2, 8, tok_dev), F32),
        pltpu.VMEM((2, 8, tok_dev), F32),
        pltpu.VMEM((2, 8, tok_dev), F32),
        dma((chunks,)), dma((chunks,)), dma((chunks,)), dma((chunks,)), dma((chunks,)), dma((chunks,)), dma, dma,
        pltpu.VMEM((8, tok_dev), F32),
        pltpu.VMEM((8, tok_dev), F32),
        pltpu.VMEM((tok_dev, width), BF16),
        pltpu.VMEM((ep, chosen, tok_dev), jnp.int32),
        pltpu.VMEM((line, packed, tok_dev), BF16),
        pltpu.VMEM((line, packed, tok_dev), BF16),
        pltpu.VMEM((line, 8, tok_dev), F32),
        pltpu.VMEM((line, 8, packed), F32),
        pltpu.VMEM((line, 8, tok_dev), F32),
        pltpu.VMEM((line, 8, packed), F32),
        pltpu.VMEM((ep, 8, tok_dev), F32),
        pltpu.VMEM((ep, 8, tok_dev), F32),
        pltpu.VMEM((dp, tok_dev, part), BF16),
        pltpu.VMEM((dp, tok_dev, part), BF16),
        pltpu.VMEM((experts, tok_dev), F32),
        pltpu.VMEM((experts, tok_dev), F32),
        pltpu.VMEM((experts, tok_dev), F32),
        pltpu.VMEM((dp, 8, experts), F32),
        pltpu.VMEM((2, 8, experts), F32),
        pltpu.VMEM((line, 8, experts), F32),
        pltpu.VMEM((dp, experts, tok_dev), BF16),
        pltpu.VMEM((ep, exp_dev, part), F32),
        pltpu.VMEM((ep, exp_dev, part), F32),
        dma, dma((chunks,)), dma((3,)), dma((ep,)),
        dma((chunks,)), dma((chunks,)), dma((line, chunks)),
        dma((chunks,)), dma((line, chunks)), dma, dma,
        dma, dma, dma, dma, dma((3,)), dma((line + 1,)),
        dma, dma, dma, dma,
    ]
    token_grad, wg, loss = pl.pallas_call(
        functools.partial(kernel, cfg),
        name="router_backward",
        out_shape=(
            jax.ShapeDtypeStruct((tok_dev, width), BF16),
            jax.ShapeDtypeStruct((exp_dev, part), F32),
            jax.ShapeDtypeStruct((1, 1), F32),
        ),
        in_specs=[hbm] * 7,
        out_specs=(hbm,) * 3,
        scratch_shapes=scratch,
        compiler_params=pltpu.CompilerParams(
            collective_id=0, has_side_effects=True, vmem_limit_bytes=56 * 1024 * 1024
        ),
    )(indices.T, out_grad, rows_t, tokens, router_weight.T, router_bias.reshape(1, experts), balance_scale.reshape(1, 1))
    return (token_grad, wg.T, loss.reshape(1))


def solution(mesh):
    placed = (
        P(("ep", "dp"), None),
        P(("ep", "dp"), None),
        P(("ep", "dp"), None),
        P("dp", "ep", None, None, None),
        P(),
        P(),
        P(),
    )
    return jax.shard_map(
        on_device,
        mesh=mesh,
        in_specs=placed,
        out_specs=(P(("ep", "dp"), None), P("dp", "ep"), P()),
        check_vma=False,
    )
```

```python
import functools
import math

import jax
import jax.numpy as jnp
from jax import lax
from jax.experimental import pallas as pl
from jax.experimental.pallas import tpu as pltpu
from jax.sharding import PartitionSpec as P

MESH = pl.DeviceIdType.MESH
F32 = jnp.float32
BF16 = jnp.bfloat16
CHUNK = 768
LAG = 4


def dot_nt(x, y, precision=None):
    return lax.dot_general(
        x, y, (((1,), (1,)), ((), ())), preferred_element_type=F32, precision=precision
    )


def dot_nn(x, y, precision=None):
    return lax.dot_general(
        x, y, (((1,), (0,)), ((), ())), preferred_element_type=F32, precision=precision
    )


def kernel(cfg, *refs):
    (ep, dp, tok_dev, chosen, experts, exp_dev, cap, packed, widths, starts, swapped, late, crossed, direct, held, token_total) = cfg
    line = ep // 2
    last = line - 1
    chunks = len(widths)
    every = range(chunks)
    kept = [c for c in every if c not in swapped]
    (idx_in, grad_in, rows_in, tok_in, wt_in, bias_in, scale_in, tg_out, wg_out, loss_out) = refs[:10]
    refs = refs[10:]
    hop = refs[5 * chunks:6 * chunks]
    hop_n = refs[6 * chunks:7 * chunks]
    back_n = refs[7 * chunks:8 * chunks]
    xb = refs[:chunks]
    lsend = refs[chunks:2 * chunks]
    lrecv = refs[2 * chunks:3 * chunks]
    rows_v = refs[3 * chunks:4 * chunks]
    back = refs[4 * chunks:5 * chunks]
    (tok_v, wt_v, bias_v, scale_v, s_in, loss_v, s_out,
     rows_raw, piled, tgt_r, acc_r, rst_r, rbuf_r, s_back, r_back, r_hop, s_near, r_hop_n, r_back_n, s_rr, r_rr, tgt_n, acc_n,
     idx_all, pin, pout, tgt_x, tgt_p, acc_x, acc_p, rst, rbuf, tks, tkr, logit_v, prob_v,
     named_v, st_dp, st_ep, lgd, ws, wr,
     s_rows, s_own, s_idx, r_idx, s_right, s_left, r_x, s_leaf, r_leaf, s_rep, r_rep,
     s_tk, r_tk, s_sd, r_sd, s_se, r_se, s_ready, s_lg, r_lg, s_w, r_w) = refs[8 * chunks:]
    me = lax.axis_index("ep")
    md = lax.axis_index("dp")
    pos = me // 2
    side = lax.rem(me, 2)
    mate = pos * 2 + 1 - side
    at_end = jnp.logical_or(pos == 0, pos == last)
    near_end = jnp.logical_or(pos == 1, pos == last - 1)
    end = jnp.where(pos * 2 < line, 0, last)
    near = jnp.where(pos * 2 < line, 1, last - 1)
    far = last - end

    def ep_id(other):
        return (other, md)

    def remote(src, dst, s, r, dev):
        return pltpu.make_async_remote_copy(
            src_ref=src, dst_ref=dst, send_sem=s, recv_sem=r, device_id=dev, device_id_type=MESH
        )

    def ep_peer(s):
        return lax.rem(me + s, ep)

    def dp_peer(s):
        return lax.rem(md + s, dp)

    barrier = pltpu.get_barrier_semaphore()

    def greet(dev):
        pl.semaphore_signal(barrier, inc=1, device_id=dev, device_id_type=MESH)

    @pl.when(pos < last)
    def _():
        greet(ep_id(me + 2))

    @pl.when(pos > 0)
    def _():
        greet(ep_id(me - 2))

    greet(ep_id(mate))
    for s in range(1, dp):
        greet((me, dp_peer(s)))

    idx_here = pltpu.make_async_copy(idx_in, idx_all.at[me], s_in.at[0])
    own = [
        pltpu.make_async_copy(grad_in.at[:, pl.ds(starts[c], widths[c])], xb[c].at[pos], s_own.at[c])
        for c in every
    ]
    rows_copy = pltpu.make_async_copy(rows_in, rows_raw, s_rows)
    small = [
        pltpu.make_async_copy(tok_in, tok_v, s_in.at[1]),
        pltpu.make_async_copy(wt_in, wt_v, s_in.at[2]),
        pltpu.make_async_copy(bias_in, bias_v, s_in.at[3]),
        pltpu.make_async_copy(scale_in, scale_v, s_in.at[4]),
    ]
    idx_here.start()
    for copy in own:
        copy.start()
    rows_copy.start()
    for copy in small:
        copy.start()
    pl.semaphore_wait(
        barrier, dp + (pos < last).astype(jnp.int32) + (pos > 0).astype(jnp.int32)
    )

    def idx_copy(q, way, dev):
        at = q * 2 + side
        return remote(idx_all.at[at], idx_all.at[at], s_idx.at[way], r_idx.at[at], ep_id(dev))

    def idx_right(q):
        return idx_copy(q, 0, me + 2)

    def idx_left(q):
        return idx_copy(q, 1, me - 2)

    def idx_mate(q):
        return idx_copy(q, 2, mate)

    def idx_from_mate(q):
        at = q * 2 + 1 - side
        return remote(idx_all.at[at], idx_all.at[at], s_idx.at[2], r_idx.at[at], ep_id(mate))

    def loop_ep(fn):
        def body(s, carry):
            fn(s)
            return carry
        lax.fori_loop(1, ep, body, 0)

    def to_right(q, c):
        return remote(xb[c].at[q], xb[c].at[q], s_right.at[c], r_x.at[q, c], ep_id(me + 2))

    def to_left(q, c):
        return remote(xb[c].at[q], xb[c].at[q], s_left.at[c], r_x.at[q - 1, c], ep_id(me - 2))

    def leaf(q, c):
        return remote(lsend[c].at[q], lrecv[c].at[q], s_leaf.at[c], r_leaf.at[q, c], ep_id(mate))

    def hop_rows(c):
        return remote(rows_v[c].at[far * 2 + 1 - side], hop[c], s_back.at[swapped.index(c)], r_hop.at[swapped.index(c)], ep_id(mate))

    def send_back(b, c):
        src = rows_v[c].at[far * 2 + side] if b == 0 else hop[c]
        at = side if b == 0 else 1 - side
        return remote(src, back[c].at[at], s_back.at[swapped.index(c)], r_back.at[swapped.index(c)], ep_id(near * 2 + side))

    def back_arrival(c):
        return remote(back[c], back[c], s_back.at[swapped.index(c)], r_back.at[swapped.index(c)], ep_id(end * 2 + side))

    def hop_near(c):
        n = crossed.index(c)
        return remote(rows_v[c].at[near * 2 + 1 - side], hop_n[c], s_near.at[n], r_hop_n.at[n], ep_id(mate))

    def send_near(c):
        n = crossed.index(c)
        if c in direct:
            return remote(rows_v[c].at[near * 2 + 1 - side], back_n[c], s_near.at[n], r_back_n.at[n], ep_id(near * 2 + 1 - side))
        return remote(hop_n[c], back_n[c], s_near.at[n], r_back_n.at[n], ep_id(near * 2 + side))

    def near_arrival(c):
        n = crossed.index(c)
        return remote(back_n[c], back_n[c], s_near.at[n], r_back_n.at[n], ep_id(end * 2 + side))

    def back_reply():
        return remote(rst_r, rbuf_r, s_rr, r_rr, ep_id(far * 2 + side))

    def back_reply_arrival():
        return remote(rst_r, rbuf_r, s_rr, r_rr, ep_id((last - near) * 2 + side))

    def reply(j):
        return remote(rst.at[j], rbuf.at[me], s_rep, r_rep, ep_id(j))

    def se_copy(s):
        return remote(st_ep.at[me], st_ep.at[me], s_se, r_se, ep_id(ep_peer(s)))

    def se_all():
        return remote(st_ep.at[pl.ds(0, ep - 1)], st_ep.at[pl.ds(0, ep - 1)], s_se, r_se, ep_id(mate))

    def say_ready(n):
        def tell(dev):
            pl.semaphore_signal(s_ready.at[n], inc=1, device_id=ep_id(dev), device_id_type=MESH)

        @pl.when(pos < last)
        def _():
            tell(me + 2)

        @pl.when(pos > 0)
        def _():
            tell(me - 2)

        tell(mate)

    def hear_ready(n):
        pl.semaphore_wait(s_ready.at[n], 1 + (pos < last).astype(jnp.int32) + (pos > 0).astype(jnp.int32))
        if n + 1 < last:
            say_ready(n + 1)

    if last > 0:
        say_ready(0)
    for copy in own:
        copy.wait()
    idx_here.wait()

    @pl.when(pos < last)
    def _():
        idx_right(pos).start()

    @pl.when(pos > 0)
    def _():
        idx_left(pos).start()

    idx_mate(pos).start()
    for c in every:
        @pl.when(pos < last - (c in late))
        def _():
            to_right(pos, c).start()

        @pl.when(pos > 0 + (c in late))
        def _():
            to_left(pos, c).start()

    expert_row = lax.broadcasted_iota(jnp.int32, (experts, tok_dev), 0)
    eye_r = lax.broadcasted_iota(jnp.int32, (experts, experts), 0)
    eye_c = lax.broadcasted_iota(jnp.int32, (experts, experts), 1)
    t_from = lax.broadcasted_iota(jnp.int32, (tok_dev, tok_dev), 0)
    t_to = lax.broadcasted_iota(jnp.int32, (tok_dev, tok_dev), 1)
    upper = jnp.where(t_from < t_to, 1.0, 0.0).astype(BF16)
    row8 = lax.broadcasted_iota(jnp.int32, (8, tok_dev), 0)
    slot_p = lax.broadcasted_iota(jnp.int32, (packed, tok_dev), 0).astype(F32)

    def upright(line_of):
        return jnp.sum(jnp.where(eye_r == eye_c, line_of, 0.0), axis=1, keepdims=True)

    def plan(table, group):
        who = jnp.where(row8 < exp_dev, group * exp_dev + row8, -2)
        hit = jnp.zeros((8, tok_dev), F32)
        for k in range(chosen):
            hit = hit + jnp.where(table[k:k + 1, :] == who, 1.0, 0.0)
        need = jnp.max(hit, axis=0, keepdims=True)
        stack = jnp.where(row8 == exp_dev, need, hit)
        before = dot_nn(stack.astype(BF16), upper)
        place = jnp.where(need > 0.5, before[exp_dev:exp_dev + 1, :], -1.0)
        target = jnp.where(hit > 0.5, before, -1.0)
        pack = jnp.where(slot_p == place, 1.0, 0.0).astype(BF16)
        return target, pack

    def plan_block(q):
        table = idx_all[q * 2 + side]
        _, pack = plan(table, mate)
        pout[q] = pack
        target, _ = plan(table, me)
        tgt_x[q] = target
        acc_x[q] = jnp.zeros((8, tok_dev), F32)

    def plan_leaf(q):
        target, pack = plan(idx_all[q * 2 + 1 - side], me)
        pin[q] = pack
        tgt_p[q] = dot_nt((target + 1.0).astype(BF16), pack) - 1.0
        acc_p[q] = jnp.zeros((8, packed), F32)

    def plan_back():
        for b in range(2):
            tgt_r[b], _ = plan(idx_all[far * 2 + side], end * 2 + b)
            acc_r[b] = jnp.zeros((8, tok_dev), F32)
        tgt_n[...], _ = plan(idx_all[me], end * 2 + 1 - side)
        acc_n[...] = jnp.zeros((8, tok_dev), F32)

    deep = piled.shape[1] // ep
    slot_r = lax.broadcasted_iota(jnp.int32, (deep, cap * ep), 0)
    lies = lax.broadcasted_iota(jnp.int32, (deep, cap * ep), 1)
    spare = rows_v[0].shape[1] - exp_dev * cap

    def sort_rows(c):
        w = widths[c]
        order = jnp.concatenate(
            [jnp.where(jnp.logical_and(lies == slot_r * ep + j, slot_r < cap), 1.0, 0.0) for j in range(ep)], axis=0
        ).astype(BF16)
        for e in range(exp_dev):
            piled[e, :, 0:w] = dot_nn(order, rows_raw[e, :, starts[c]:starts[c] + w])

        def put(j, carry):
            at = pl.ds(pl.multiple_of(j * deep, 8), deep)
            pieces = [piled[e, at, 0:w][0:cap, :] for e in range(exp_dev)]
            if spare:
                pieces.append(jnp.zeros((spare, w), F32))
            rows_v[c][j] = jnp.concatenate(pieces, axis=0).astype(BF16)
            return carry

        lax.fori_loop(0, ep, put, 0)

    def gathered(table, block, target, count):
        height = table.shape[0]
        slot = lax.broadcasted_iota(jnp.int32, (height, count), 0).astype(F32)
        row = lax.broadcasted_iota(jnp.int32, (8, count), 0)
        dots = dot_nt(table, block)
        out = jnp.zeros((8, count), F32)
        for e in range(exp_dev):
            want = jnp.where(target[e:e + 1, :] >= 0.0, target[e:e + 1, :] + e * cap, -1.0)
            one = jnp.sum(jnp.where(slot == want, dots, 0.0), axis=0, keepdims=True)
            out = jnp.where(row == e, one, out)
        return out

    def give_leaf(q, c):
        lsend[c][q] = dot_nn(pout[q], xb[c][q]).astype(BF16)
        leaf(q, c).start()

    def use_block(q, c):
        acc_x[q] += gathered(rows_v[c][q * 2 + side], xb[c][q], tgt_x[q], tok_dev)

    def use_leaf(q, c):
        leaf(q, c).wait_recv()
        acc_p[q] += gathered(rows_v[c][q * 2 + 1 - side], lrecv[c][q], tgt_p[q], packed)

    def answer(j, value):
        rst[j] = value
        reply(j).start()

    def done_block(q):
        answer(q * 2 + side, acc_x[q])

    def done_leaf(q):
        answer(q * 2 + 1 - side, dot_nn(acc_p[q], pin[q].astype(F32), lax.Precision.HIGHEST))

    def meets(s, c, tail):
        left, right = pos - s >= 0, pos + s < line
        if s == last and c in swapped:
            return ()
        if s == 1 and c in late:
            inner = at_end if tail else jnp.logical_not(at_end)
            left, right = jnp.logical_and(left, inner), jnp.logical_and(right, inner)
        return ((pos - s, left, True), (pos + s, right, False))

    def closes(s, c, tail, finish, q):
        if s == 1 and len(late):
            ends = [n for n in late if finish is done_block or n not in crossed]
            if tail:
                if c == ends[-1]:
                    finish(q)
            elif c == chunks - 1:
                @pl.when(jnp.logical_not(at_end))
                def _():
                    finish(q)
        elif c == (kept[-1] if s == last else chunks - 1):
            finish(q)

    def learn(s):
        for q, ok, rightward in ((pos - s, pos - s >= 0, True), (pos + s, pos + s < line, False)):
            @pl.when(ok)
            def _(q=q, rightward=rightward):
                step = idx_right if rightward else idx_left
                step(q).wait_recv()

                @pl.when(pos < last if rightward else pos > 0)
                def _():
                    step(q).start()
                    if s == last - 1 and len(swapped):
                        plan_back()

                idx_mate(q).start()
                plan_block(q)

    def learn_leaf(s):
        for q, ok in ((pos - s, pos - s >= 0), (pos + s, pos + s < line))[:1 if s == 0 else 2]:
            @pl.when(ok)
            def _(q=q):
                idx_from_mate(q).wait_recv()
                plan_leaf(q)

    def arrive(s, c, tail=False):
        for q, ok, rightward in meets(s, c, tail):
            @pl.when(ok)
            def _(q=q, rightward=rightward):
                step = to_right if rightward else to_left
                step(q, c).wait_recv()

                @pl.when(pos < last if rightward else pos > 0)
                def _():
                    if not (s == last - 1 and c in swapped):
                        step(q, c).start()
                    if s == last - 1 and c == kept[-1]:
                        for n in late:
                            step(pos, n).start()

                if not (tail and c in crossed):
                    give_leaf(q, c)
                if s == last - 1 and c == chunks - 1 and len(held):
                    @pl.when(pos < last if rightward else pos > 0)
                    def _():
                        for n in held:
                            give_leaf(pos, n)

    def use(s, c, tail=False):
        for q, ok, rightward in meets(s, c, tail):
            @pl.when(ok)
            def _(q=q, rightward=rightward):
                use_block(q, c)
                closes(s, c, tail, done_block, q)
                if s == last - 1 and c in swapped:
                    @pl.when(pos < last if rightward else pos > 0)
                    def _():
                        back_arrival(c).wait_recv()
                        for b in range(2):
                            acc_r[b] += gathered(back[c][b], xb[c][q], tgt_r[b], tok_dev)
                        if c == swapped[-1]:
                            rst_r[...] = acc_r[...]
                            back_reply().start()
                            for n in crossed:
                                near_arrival(n).wait_recv()
                                acc_n[...] += gathered(back_n[n][...], xb[n][pos], tgt_n[...], tok_dev)

    def take(s, c, tail=False):
        if s == 0:
            if len(held) and (c in held or c == chunks - 1):
                if c not in held:
                    use_leaf(pos, c)

                @pl.when(near_end if tail else jnp.logical_not(near_end))
                def _():
                    if c in held:
                        use_leaf(pos, c)
                    if c == (held[-1] if tail else chunks - 1):
                        done_leaf(pos)
            else:
                use_leaf(pos, c)
                if c == chunks - 1:
                    done_leaf(pos)
            return
        for q, ok, _ in meets(s, c, tail):
            @pl.when(ok)
            def _(q=q):
                use_leaf(q, c)
                closes(s, c, tail, done_leaf, q)

    def settle(s, c):
        if c == 0:
            learn_leaf(s)
        take(s, c)

    def pass_rows(c):
        @pl.when(at_end)
        def _():
            if c in swapped:
                hop_rows(c).wait_recv()
                send_back(1, c).start()
            if c in crossed and c not in direct:
                hop_near(c).wait_recv()
                send_near(c).start()

    def sort_step(c):
        sort_rows(c)
        if c in swapped or c in crossed:
            @pl.when(at_end)
            def _():
                if c in swapped:
                    hop_rows(c).start()
                    send_back(0, c).start()
                if c in direct:
                    send_near(c).start()
                elif c in crossed:
                    hop_near(c).start()
        use_block(pos, c)
        if c == chunks - 1:
            rbuf[me] = acc_x[pos]

    part = tok_in.shape[1] // dp

    def tk_copy(s):
        return remote(tks.at[dp_peer(s)], tkr.at[md], s_tk, r_tk, (me, dp_peer(s)))

    def tk_all():
        return remote(tks.at[pl.ds(0, dp - 1)], tkr.at[pl.ds(0, dp - 1)], s_tk, r_tk, (me, dp_peer(1)))

    def sd_copy(s):
        return remote(st_dp.at[md], st_dp.at[md], s_sd, r_sd, (me, dp_peer(s)))

    def sd_all():
        return remote(st_dp.at[pl.ds(0, dp - 1)], st_dp.at[pl.ds(0, dp - 1)], s_sd, r_sd, (me, dp_peer(1)))

    def route():
        for copy in small:
            copy.wait()
        idx = idx_all[me]
        named = jnp.zeros((experts, tok_dev), F32)
        for k in range(chosen):
            named = named + jnp.where(idx[k:k + 1, :] == expert_row, 1.0, 0.0)
        logits = dot_nt(wt_v[...], tok_v[...]) + upright(bias_v[...])
        top = jnp.max(logits, axis=0, keepdims=True)
        power = jnp.exp(logits - top)
        prob = power / jnp.sum(power, axis=0, keepdims=True)
        logit_v[...] = logits
        prob_v[...] = prob
        named_v[...] = named
        ones = jnp.ones((8, tok_dev), F32)
        count_row = dot_nt(ones, named, lax.Precision.HIGHEST)
        prob_row = dot_nt(ones, prob, lax.Precision.HIGHEST)
        stat_row = lax.broadcasted_iota(jnp.int32, (8, experts), 0)
        st_dp[md] = jnp.where(stat_row == 0, count_row, prob_row)
        for s in range(1, dp):
            sd_copy(s).start()

    def share_tokens():
        for d in range(dp):
            tks[d] = tok_v[:, d * part:(d + 1) * part]
        for s in range(1, dp):
            tk_copy(s).start()
        tkr[md] = tks[md]

    def share_stats():
        sd_all().wait_recv()
        total = st_dp[0]
        for d in range(1, dp):
            total = total + st_dp[d]
        st_ep[me] = total
        loop_ep(lambda s: se_copy(s).start())

    plan_block(pos)
    for c in every:
        if c in held:
            @pl.when(jnp.logical_not(near_end))
            def _():
                give_leaf(pos, c)
        else:
            give_leaf(pos, c)
    rows_copy.wait()
    for c in every:
        if c == max(chunks - 2, 0):
            learn(1)
            arrive(1, 0)
        sort_step(c)
        if c < last:
            hear_ready(c)
    for n in range(chunks, last):
        hear_ready(n)
    steps = [(0, c) for c in every] + [(s, c) for s in range(1, line) for c in every]
    taken, tails = 0, []
    for n, (s, c) in enumerate(steps):
        if s == last and c in swapped:
            break
        if s > 0:
            if c == 0:
                if s > 1:
                    learn(s)
            if (s, c) != (1, 0):
                arrive(s, c)
            use(s, c)
            if (s, c) == (2, 0):
                for n in every:
                    if n in swapped or n in crossed:
                        pass_rows(n)
            if (s, c) == (1, 1 if chunks > 1 else 0):
                route()
                share_tokens()
            if (s, c) == (1, chunks - 1):
                share_stats()
            while taken <= n - LAG:
                settle(*steps[taken])
                taken += 1
    for c in late:
        arrive(1, c, True)
        use(1, c, True)
        for step in steps[taken:taken + 2]:
            settle(*step)
        taken = min(taken + 2, len(steps))
        if c not in crossed:
            tails.append(c)
    for step in steps[taken:]:
        settle(*step)
    for c in held:
        take(0, c, True)
    for c in tails:
        take(1, c, True)
    se_all().wait_recv()
    stats = lax.fori_loop(1, ep, lambda j, acc: acc + st_ep[j], st_ep[0])
    share = stats[0:1, :] / (token_total * chosen)
    mean = stats[1:2, :] / token_total
    loss_v[...] = experts * jnp.sum(share * mean, axis=1, keepdims=True)
    loss_copy = pltpu.make_async_copy(loss_v, loss_out, s_out)
    loss_copy.start()
    push_row = scale_v[...] * experts * share
    push = upright(push_row)
    prob = prob_v[...]
    spread = prob * (push - jnp.sum(prob * push, axis=0, keepdims=True))
    named = named_v[...]
    logits = logit_v[...]
    high = jnp.max(jnp.where(named > 0.5, logits, -jnp.inf), axis=0, keepdims=True)
    mix = jnp.where(named > 0.5, jnp.exp(jnp.minimum(logits - high, 0.0)), 0.0)
    mix = mix / jnp.sum(mix, axis=0, keepdims=True)

    remote(rst.at[pl.ds(0, ep - 1)], rbuf.at[pl.ds(0, ep - 1)], s_rep, r_rep, ep_id(mate)).wait_recv()
    if len(swapped):
        @pl.when(at_end)
        def _():
            back_reply_arrival().wait_recv()
            for b in range(2):
                rbuf[far * 2 + b] += rbuf_r[b]

        @pl.when(near_end)
        def _():
            rbuf[end * 2 + 1 - side] += acc_n[...]
    dots = jnp.concatenate([rbuf[j, 0:exp_dev, :] for j in range(ep)], axis=0)
    sel = mix * (dots - jnp.sum(mix * dots, axis=0, keepdims=True))
    grad = (spread + sel).astype(BF16)
    lgd[md] = grad

    def lg_copy(s):
        return remote(lgd.at[md], lgd.at[md], s_lg, r_lg, (me, dp_peer(s)))

    def lg_all():
        return remote(lgd.at[pl.ds(0, dp - 1)], lgd.at[pl.ds(0, dp - 1)], s_lg, r_lg, (me, dp_peer(1)))

    for s in range(1, dp):
        lg_copy(s).start()
    for c in every:
        at = slice(starts[c], starts[c] + widths[c])
        tg_out[:, at] = lax.dot_general(
            grad, wt_v[:, at], (((0,), (0,)), ((), ())), preferred_element_type=F32
        ).astype(BF16)
    tk_all().wait_recv()
    lg_all().wait_recv()
    term = dot_nn(lgd[0], tkr[0])
    for d in range(1, dp):
        term = term + dot_nn(lgd[d], tkr[d])
    for j in range(ep):
        ws[j] = term[j * exp_dev:(j + 1) * exp_dev, :]
    wr[me] = ws[me]

    def w_copy(s_):
        return remote(ws.at[ep_peer(s_)], wr.at[me], s_w, r_w, ep_id(ep_peer(s_)))

    def w_all():
        return remote(ws.at[pl.ds(0, ep - 1)], wr.at[pl.ds(0, ep - 1)], s_w, r_w, ep_id(mate))

    loop_ep(lambda s_: w_copy(s_).start())

    def sent(ref, sem, count):
        for n in range(1, line + 1):
            @pl.when(count == n)
            def _(n=n):
                piece = ref.at[pl.ds(0, n)]
                remote(piece, piece, sem, sem, ep_id(mate)).wait_send()

    ups = jnp.where(pos < last, pos + 1, 0)
    downs = jnp.where(pos > 0, line - pos, 0)
    sent(idx_all, s_idx.at[0], ups)
    sent(idx_all, s_idx.at[1], downs)
    sent(idx_all, s_idx.at[2], line)
    se_all().wait_send()
    for c in every:
        short = 1 if c in swapped else 0
        sent(xb[c], s_right.at[c], ups - jnp.where(pos == last - 1, short, 0))
        sent(xb[c], s_left.at[c], downs - jnp.where(pos == 1, short, 0))
        skipped = short + (1 if c in crossed else 0)
        sent(lsend[c], s_leaf.at[c], line - jnp.where(at_end, skipped, 0))
    if len(swapped):
        @pl.when(at_end)
        def _():
            for c in swapped:
                piece = rows_v[c].at[pl.ds(0, 3)]
                sem = s_back.at[swapped.index(c)]
                remote(piece, piece, sem, sem, ep_id(mate)).wait_send()
            for n, c in enumerate(crossed):
                piece = rows_v[c].at[pl.ds(0, 1 if c in direct else 2)]
                remote(piece, piece, s_near.at[n], s_near.at[n], ep_id(mate)).wait_send()

        @pl.when(near_end)
        def _():
            back_reply().wait_send()
    remote(rst.at[pl.ds(0, ep - 1)], rbuf.at[pl.ds(0, ep - 1)], s_rep, r_rep, ep_id(mate)).wait_send()
    sd_all().wait_send()
    tk_all().wait_send()
    lg_all().wait_send()
    loss_copy.wait()
    w_all().wait_recv()
    out = lax.fori_loop(1, ep, lambda j, acc: acc + wr[j], wr[0])
    wg_out[...] = out / math.sqrt(token_total)
    w_all().wait_send()


def cut(width):
    if width <= 3 * CHUNK + CHUNK // 2 or width > 4 * CHUNK:
        widths = tuple(min(CHUNK, width - s) for s in range(0, width, CHUNK))
        return widths, tuple(sum(widths[:c]) for c in range(len(widths))), (), (), (), (), ()
    half = CHUNK // 2
    rest = width - 3 * CHUNK - half
    return (CHUNK, rest, half, CHUNK, CHUNK), (0, width - rest, CHUNK, CHUNK + half, 2 * CHUNK + half), (2, 3, 4), (4, 2, 1), (2, 1), (2,), (3,)


def on_device(tokens, out_grad, indices, expert_rows, router_weight, router_bias, balance_scale):
    tok_dev, width = tokens.shape
    chosen = indices.shape[1]
    experts = router_weight.shape[1]
    exp_dev, cap = expert_rows.shape[1], expert_rows.shape[3]
    ep = lax.axis_size("ep")
    dp = lax.axis_size("dp")
    line = ep // 2
    packed = -(-min(tok_dev, (exp_dev - 1) * cap) // 16) * 16
    widths, starts, swapped, late, crossed, direct, held = cut(width)
    chunks = len(widths)
    if line < 4:
        swapped, late, crossed, direct, held = (), (), (), (), ()
    cfg = (ep, dp, tok_dev, chosen, experts, exp_dev, cap, packed, widths, starts, swapped, late, crossed, direct, held, tok_dev * ep * dp)
    part = width // dp
    rows_t = jnp.transpose(expert_rows[0], (0, 2, 1, 3)).reshape(exp_dev, cap * ep, width)
    hbm = pl.BlockSpec(memory_space=pl.ANY)
    vmem = pl.BlockSpec(memory_space=pltpu.VMEM)
    dma = pltpu.SemaphoreType.DMA
    scratch = [pltpu.VMEM((line, tok_dev, w), BF16) for w in widths]
    scratch += [pltpu.VMEM((line, packed, w), BF16) for w in widths]
    scratch += [pltpu.VMEM((line, packed, w), BF16) for w in widths]
    scratch += [pltpu.VMEM((ep, -(-exp_dev * cap // 16) * 16, w), BF16) for w in widths]
    scratch += [pltpu.VMEM((2, -(-exp_dev * cap // 16) * 16, w), BF16) for w in widths]
    scratch += [pltpu.VMEM((-(-exp_dev * cap // 16) * 16, w), BF16) for w in widths]
    scratch += [pltpu.VMEM((-(-exp_dev * cap // 16) * 16, w), BF16) for w in widths]
    scratch += [pltpu.VMEM((-(-exp_dev * cap // 16) * 16, w), BF16) for w in widths]
    scratch += [
        pltpu.VMEM((tok_dev, width), BF16),
        pltpu.VMEM((experts, width), BF16),
        pltpu.VMEM((1, experts), F32),
        pltpu.VMEM((1, 1), F32),
        dma((5,)),
        pltpu.VMEM((1, 1), F32),
        dma,
        pltpu.VMEM((exp_dev, cap * ep, width), BF16),
        pltpu.VMEM((exp_dev, ep * (-(-cap // 8) * 8), max(widths)), F32),
        pltpu.VMEM((2, 8, tok_dev), F32),
        pltpu.VMEM((2, 8, tok_dev), F32),
        pltpu.VMEM((2, 8, tok_dev), F32),
        pltpu.VMEM((2, 8, tok_dev), F32),
        *[dma((max(len(swapped), 1),))] * 3, *[dma((max(len(crossed), 1),))] * 3, dma, dma,
        pltpu.VMEM((8, tok_dev), F32),
        pltpu.VMEM((8, tok_dev), F32),
        pltpu.VMEM((ep, chosen, tok_dev), jnp.int32),
        pltpu.VMEM((line, packed, tok_dev), BF16),
        pltpu.VMEM((line, packed, tok_dev), BF16),
        pltpu.VMEM((line, 8, tok_dev), F32),
        pltpu.VMEM((line, 8, packed), F32),
        pltpu.VMEM((line, 8, tok_dev), F32),
        pltpu.VMEM((line, 8, packed), F32),
        pltpu.VMEM((ep, 8, tok_dev), F32),
        pltpu.VMEM((ep, 8, tok_dev), F32),
        pltpu.VMEM((dp, tok_dev, part), BF16),
        pltpu.VMEM((dp, tok_dev, part), BF16),
        pltpu.VMEM((experts, tok_dev), F32),
        pltpu.VMEM((experts, tok_dev), F32),
        pltpu.VMEM((experts, tok_dev), F32),
        pltpu.VMEM((dp, 8, experts), F32),
        pltpu.VMEM((ep, 8, experts), F32),
        pltpu.VMEM((dp, experts, tok_dev), BF16),
        pltpu.VMEM((ep, exp_dev, part), F32),
        pltpu.VMEM((ep, exp_dev, part), F32),
        dma, dma((chunks,)), dma((3,)), dma((ep,)),
        dma((chunks,)), dma((chunks,)), dma((max(line - 1, 1), chunks)),
        dma((chunks,)), dma((line, chunks)), dma, dma,
        dma, dma, dma, dma, dma, dma, pltpu.SemaphoreType.REGULAR((max(line - 1, 1),)),
        dma, dma, dma, dma,
    ]
    token_grad, wg, loss = pl.pallas_call(
        functools.partial(kernel, cfg),
        name="router_backward",
        out_shape=(
            pltpu.VMEM((tok_dev, width), BF16),
            pltpu.VMEM((exp_dev, part), F32),
            jax.ShapeDtypeStruct((1, 1), F32),
        ),
        in_specs=[hbm] * 7,
        out_specs=(vmem, vmem, hbm),
        scratch_shapes=scratch,
        compiler_params=pltpu.CompilerParams(
            collective_id=0, has_side_effects=True, vmem_limit_bytes=56 * 1024 * 1024
        ),
    )(indices.T, out_grad, rows_t, tokens, router_weight.T, router_bias.reshape(1, experts), balance_scale.reshape(1, 1))
    return (token_grad, wg.T, loss.reshape(1))


def solution(mesh):
    placed = (
        P(("ep", "dp"), None),
        P(("ep", "dp"), None),
        P(("ep", "dp"), None),
        P("dp", "ep", None, None, None),
        P(),
        P(),
        P(),
    )
    return jax.shard_map(
        on_device,
        mesh=mesh,
        in_specs=placed,
        out_specs=(P(("ep", "dp"), None), P("dp", "ep"), P()),
        check_vma=False,
    )
```

```python
import functools
import math

import jax
import jax.numpy as jnp
from jax import lax
from jax.experimental import pallas as pl
from jax.experimental.pallas import tpu as pltpu
from jax.sharding import PartitionSpec as P

MESH = pl.DeviceIdType.MESH
F32 = jnp.float32
BF16 = jnp.bfloat16
CHUNK = 768
LAG = 4


def dot_nt(x, y, precision=None):
    return lax.dot_general(
        x, y, (((1,), (1,)), ((), ())), preferred_element_type=F32, precision=precision
    )


def dot_nn(x, y, precision=None):
    return lax.dot_general(
        x, y, (((1,), (0,)), ((), ())), preferred_element_type=F32, precision=precision
    )


def fold(left, right):
    half = right.shape[0] // 2
    pieces = [left, jnp.concatenate([right[0:half], right[half:]], axis=1)]
    short = -3 * half % 16
    if short:
        pieces.append(jnp.zeros((short, 128), F32))
    return jnp.concatenate(pieces, axis=0)


def unfold(x, rows):
    low = x[rows:, :].astype(F32)[0:rows // 2]
    return x[0:rows], jnp.concatenate([low[:, 0:64], low[:, 64:128]], axis=0).astype(BF16)


def kernel(cfg, *refs):
    (ep, dp, tok_dev, chosen, experts, exp_dev, cap, packed, widths, starts, swapped, late, crossed, direct, held, folded, token_total) = cfg
    line = ep // 2
    last = line - 1
    chunks = len(widths)
    every = range(chunks)
    kept = [c for c in every if c not in swapped]
    (idx_in, grad_in, rows_in, tok_in, wt_in, bias_in, scale_in, tg_out, wg_out, loss_out) = refs[:10]
    refs = refs[10:]
    hop = refs[5 * chunks:6 * chunks]
    hop_n = refs[6 * chunks:7 * chunks]
    back_n = refs[7 * chunks:8 * chunks]
    xb = refs[:chunks]
    lsend = refs[chunks:2 * chunks]
    lrecv = refs[2 * chunks:3 * chunks]
    rows_v = refs[3 * chunks:4 * chunks]
    back = refs[4 * chunks:5 * chunks]
    (tok_v, wt_v, bias_v, scale_v, s_in, loss_v, s_out, stage,
     rows_raw, piled, tgt_r, acc_r, rst_r, rbuf_r, s_back, r_back, r_hop, s_near, r_hop_n, r_back_n, s_rr, r_rr, tgt_n, acc_n,
     idx_all, pin, pout, tgt_x, tgt_p, acc_x, acc_p, rst, rbuf, tks, tkr, logit_v, prob_v,
     named_v, st_dp, st_ep, lgd, ws, wr,
     s_rows, s_own, s_idx, r_idx, s_right, s_left, r_x, s_leaf, r_leaf, s_rep, r_rep,
     s_tk, r_tk, s_sd, r_sd, s_se, r_se, s_ready, s_lg, r_lg, s_w, r_w) = refs[8 * chunks:]
    me = lax.axis_index("ep")
    md = lax.axis_index("dp")
    pos = me // 2
    side = lax.rem(me, 2)
    mate = pos * 2 + 1 - side
    at_end = jnp.logical_or(pos == 0, pos == last)
    near_end = jnp.logical_or(pos == 1, pos == last - 1)
    end = jnp.where(pos * 2 < line, 0, last)
    near = jnp.where(pos * 2 < line, 1, last - 1)
    far = last - end

    def ep_id(other):
        return (other, md)

    def remote(src, dst, s, r, dev):
        return pltpu.make_async_remote_copy(
            src_ref=src, dst_ref=dst, send_sem=s, recv_sem=r, device_id=dev, device_id_type=MESH
        )

    def ep_peer(s):
        return lax.rem(me + s, ep)

    def dp_peer(s):
        return lax.rem(md + s, dp)

    barrier = pltpu.get_barrier_semaphore()

    def greet(dev):
        pl.semaphore_signal(barrier, inc=1, device_id=dev, device_id_type=MESH)

    @pl.when(pos < last)
    def _():
        greet(ep_id(me + 2))

    @pl.when(pos > 0)
    def _():
        greet(ep_id(me - 2))

    greet(ep_id(mate))
    for s in range(1, dp):
        greet((me, dp_peer(s)))

    idx_here = pltpu.make_async_copy(idx_in, idx_all.at[me], s_in.at[0])
    own = [
        pltpu.make_async_copy(
            grad_in.at[:, pl.ds(starts[c], widths[c])], stage if c in folded else xb[c].at[pos], s_own.at[c]
        )
        for c in every
    ]
    rows_copy = pltpu.make_async_copy(rows_in, rows_raw, s_rows)
    small = [
        pltpu.make_async_copy(tok_in, tok_v, s_in.at[1]),
        pltpu.make_async_copy(wt_in, wt_v, s_in.at[2]),
        pltpu.make_async_copy(bias_in, bias_v, s_in.at[3]),
        pltpu.make_async_copy(scale_in, scale_v, s_in.at[4]),
    ]
    idx_here.start()
    for copy in own:
        copy.start()
    rows_copy.start()
    for copy in small:
        copy.start()
    pl.semaphore_wait(
        barrier, dp + (pos < last).astype(jnp.int32) + (pos > 0).astype(jnp.int32)
    )

    def idx_copy(q, way, dev):
        at = q * 2 + side
        return remote(idx_all.at[at], idx_all.at[at], s_idx.at[way], r_idx.at[at], ep_id(dev))

    def idx_right(q):
        return idx_copy(q, 0, me + 2)

    def idx_left(q):
        return idx_copy(q, 1, me - 2)

    def idx_mate(q):
        return idx_copy(q, 2, mate)

    def idx_from_mate(q):
        at = q * 2 + 1 - side
        return remote(idx_all.at[at], idx_all.at[at], s_idx.at[2], r_idx.at[at], ep_id(mate))

    def loop_ep(fn):
        def body(s, carry):
            fn(s)
            return carry
        lax.fori_loop(1, ep, body, 0)

    def to_right(q, c):
        return remote(xb[c].at[q], xb[c].at[q], s_right.at[c], r_x.at[q, c], ep_id(me + 2))

    def to_left(q, c):
        return remote(xb[c].at[q], xb[c].at[q], s_left.at[c], r_x.at[q - 1, c], ep_id(me - 2))

    def leaf(q, c):
        return remote(lsend[c].at[q], lrecv[c].at[q], s_leaf.at[c], r_leaf.at[q, c], ep_id(mate))

    def hop_rows(c):
        return remote(rows_v[c].at[far * 2 + 1 - side], hop[c], s_back.at[swapped.index(c)], r_hop.at[swapped.index(c)], ep_id(mate))

    def send_back(b, c):
        src = rows_v[c].at[far * 2 + side] if b == 0 else hop[c]
        at = side if b == 0 else 1 - side
        return remote(src, back[c].at[at], s_back.at[swapped.index(c)], r_back.at[swapped.index(c)], ep_id(near * 2 + side))

    def back_arrival(c):
        return remote(back[c], back[c], s_back.at[swapped.index(c)], r_back.at[swapped.index(c)], ep_id(end * 2 + side))

    def hop_near(c):
        n = crossed.index(c)
        return remote(rows_v[c].at[near * 2 + 1 - side], hop_n[c], s_near.at[n], r_hop_n.at[n], ep_id(mate))

    def send_near(c):
        n = crossed.index(c)
        if c in direct:
            return remote(rows_v[c].at[near * 2 + 1 - side], back_n[c], s_near.at[n], r_back_n.at[n], ep_id(near * 2 + 1 - side))
        return remote(hop_n[c], back_n[c], s_near.at[n], r_back_n.at[n], ep_id(near * 2 + side))

    def near_arrival(c):
        n = crossed.index(c)
        return remote(back_n[c], back_n[c], s_near.at[n], r_back_n.at[n], ep_id(end * 2 + side))

    def back_reply():
        return remote(rst_r, rbuf_r, s_rr, r_rr, ep_id(far * 2 + side))

    def back_reply_arrival():
        return remote(rst_r, rbuf_r, s_rr, r_rr, ep_id((last - near) * 2 + side))

    def reply(j):
        return remote(rst.at[j], rbuf.at[me], s_rep, r_rep, ep_id(j))

    def se_copy(s):
        return remote(st_ep.at[me], st_ep.at[me], s_se, r_se, ep_id(ep_peer(s)))

    def se_all():
        return remote(st_ep.at[pl.ds(0, ep - 1)], st_ep.at[pl.ds(0, ep - 1)], s_se, r_se, ep_id(mate))

    def say_ready(n):
        def tell(dev):
            pl.semaphore_signal(s_ready.at[n], inc=1, device_id=ep_id(dev), device_id_type=MESH)

        @pl.when(pos < last)
        def _():
            tell(me + 2)

        @pl.when(pos > 0)
        def _():
            tell(me - 2)

        tell(mate)

    def hear_ready(n):
        pl.semaphore_wait(s_ready.at[n], 1 + (pos < last).astype(jnp.int32) + (pos > 0).astype(jnp.int32))
        if n + 1 < last:
            say_ready(n + 1)

    if last > 0:
        say_ready(0)
    for copy in own:
        copy.wait()
    idx_here.wait()

    @pl.when(pos < last)
    def _():
        idx_right(pos).start()

    @pl.when(pos > 0)
    def _():
        idx_left(pos).start()

    idx_mate(pos).start()
    for c in every:
        if c in folded:
            xb[c][pos] = fold(stage[:, 0:128].astype(F32), stage[:, 128:192].astype(F32)).astype(BF16)

        @pl.when(pos < last - (c in late))
        def _():
            to_right(pos, c).start()

        @pl.when(pos > 0 + (c in late))
        def _():
            to_left(pos, c).start()

    expert_row = lax.broadcasted_iota(jnp.int32, (experts, tok_dev), 0)
    eye_r = lax.broadcasted_iota(jnp.int32, (experts, experts), 0)
    eye_c = lax.broadcasted_iota(jnp.int32, (experts, experts), 1)
    t_from = lax.broadcasted_iota(jnp.int32, (tok_dev, tok_dev), 0)
    t_to = lax.broadcasted_iota(jnp.int32, (tok_dev, tok_dev), 1)
    upper = jnp.where(t_from < t_to, 1.0, 0.0).astype(BF16)
    row8 = lax.broadcasted_iota(jnp.int32, (8, tok_dev), 0)
    slot_p = lax.broadcasted_iota(jnp.int32, (packed, tok_dev), 0).astype(F32)

    def upright(line_of):
        return jnp.sum(jnp.where(eye_r == eye_c, line_of, 0.0), axis=1, keepdims=True)

    def plan(table, group):
        who = jnp.where(row8 < exp_dev, group * exp_dev + row8, -2)
        hit = jnp.zeros((8, tok_dev), F32)
        for k in range(chosen):
            hit = hit + jnp.where(table[k:k + 1, :] == who, 1.0, 0.0)
        need = jnp.max(hit, axis=0, keepdims=True)
        stack = jnp.where(row8 == exp_dev, need, hit)
        before = dot_nn(stack.astype(BF16), upper)
        place = jnp.where(need > 0.5, before[exp_dev:exp_dev + 1, :], -1.0)
        target = jnp.where(hit > 0.5, before, -1.0)
        pack = jnp.where(slot_p == place, 1.0, 0.0).astype(BF16)
        return target, pack

    def plan_block(q):
        table = idx_all[q * 2 + side]
        _, pack = plan(table, mate)
        pout[q] = pack
        target, _ = plan(table, me)
        tgt_x[q] = target
        acc_x[q] = jnp.zeros((8, tok_dev), F32)

    def plan_leaf(q):
        target, pack = plan(idx_all[q * 2 + 1 - side], me)
        pin[q] = pack
        tgt_p[q] = dot_nt((target + 1.0).astype(BF16), pack) - 1.0
        acc_p[q] = jnp.zeros((8, packed), F32)

    def plan_back():
        for b in range(2):
            tgt_r[b], _ = plan(idx_all[far * 2 + side], end * 2 + b)
            acc_r[b] = jnp.zeros((8, tok_dev), F32)
        tgt_n[...], _ = plan(idx_all[me], end * 2 + 1 - side)
        acc_n[...] = jnp.zeros((8, tok_dev), F32)

    deep = piled.shape[1] // ep
    slot_r = lax.broadcasted_iota(jnp.int32, (deep, cap * ep), 0)
    lies = lax.broadcasted_iota(jnp.int32, (deep, cap * ep), 1)
    spare = -exp_dev * cap % 16

    def sort_rows(c):
        w = widths[c]
        order = jnp.concatenate(
            [jnp.where(jnp.logical_and(lies == slot_r * ep + j, slot_r < cap), 1.0, 0.0) for j in range(ep)], axis=0
        ).astype(BF16)
        for e in range(exp_dev):
            piled[e, :, 0:w] = dot_nn(order, rows_raw[e, :, starts[c]:starts[c] + w])

        def put(j, carry):
            at = pl.ds(pl.multiple_of(j * deep, 8), deep)
            pieces = [piled[e, at, 0:w][0:cap, :] for e in range(exp_dev)]
            if spare:
                pieces.append(jnp.zeros((spare, w), F32))
            block = jnp.concatenate(pieces, axis=0)
            if c in folded:
                block = fold(block[:, 0:128], block[:, 128:192])
            rows_v[c][j] = block.astype(BF16)
            return carry

        lax.fori_loop(0, ep, put, 0)

    def all_dots(c, table, block, count):
        if c not in folded:
            return dot_nt(table, block)
        (table_l, table_r), (block_l, block_r) = unfold(table, exp_dev * cap + spare), unfold(block, count)
        return dot_nt(table_l, block_l) + dot_nt(table_r, block_r)

    def gathered(c, table, block, target, count):
        dots = all_dots(c, table, block, count)
        height = dots.shape[0]
        slot = lax.broadcasted_iota(jnp.int32, (height, count), 0).astype(F32)
        row = lax.broadcasted_iota(jnp.int32, (8, count), 0)
        out = jnp.zeros((8, count), F32)
        for e in range(exp_dev):
            want = jnp.where(target[e:e + 1, :] >= 0.0, target[e:e + 1, :] + e * cap, -1.0)
            one = jnp.sum(jnp.where(slot == want, dots, 0.0), axis=0, keepdims=True)
            out = jnp.where(row == e, one, out)
        return out

    def give_leaf(q, c):
        if c in folded:
            left, right = unfold(xb[c][q], tok_dev)
            lsend[c][q] = fold(dot_nn(pout[q], left), dot_nn(pout[q], right)).astype(BF16)
        else:
            lsend[c][q] = dot_nn(pout[q], xb[c][q]).astype(BF16)
        leaf(q, c).start()

    def use_block(q, c):
        acc_x[q] += gathered(c, rows_v[c][q * 2 + side], xb[c][q], tgt_x[q], tok_dev)

    def use_leaf(q, c):
        leaf(q, c).wait_recv()
        acc_p[q] += gathered(c, rows_v[c][q * 2 + 1 - side], lrecv[c][q], tgt_p[q], packed)

    def answer(j, value):
        rst[j] = value
        reply(j).start()

    def done_block(q):
        answer(q * 2 + side, acc_x[q])

    def done_leaf(q):
        answer(q * 2 + 1 - side, dot_nn(acc_p[q], pin[q].astype(F32), lax.Precision.HIGHEST))

    def meets(s, c, tail):
        left, right = pos - s >= 0, pos + s < line
        if s == last and c in swapped:
            return ()
        if s == 1 and c in late:
            inner = at_end if tail else jnp.logical_not(at_end)
            left, right = jnp.logical_and(left, inner), jnp.logical_and(right, inner)
        return ((pos - s, left, True), (pos + s, right, False))

    def closes(s, c, tail, finish, q):
        if s == 1 and len(late):
            ends = [n for n in late if finish is done_block or n not in crossed]
            if tail:
                if c == ends[-1]:
                    finish(q)
            elif c == chunks - 1:
                @pl.when(jnp.logical_not(at_end))
                def _():
                    finish(q)
        elif c == (kept[-1] if s == last else chunks - 1):
            finish(q)

    def learn(s):
        for q, ok, rightward in ((pos - s, pos - s >= 0, True), (pos + s, pos + s < line, False)):
            @pl.when(ok)
            def _(q=q, rightward=rightward):
                step = idx_right if rightward else idx_left
                step(q).wait_recv()

                @pl.when(pos < last if rightward else pos > 0)
                def _():
                    step(q).start()
                    if s == last - 1 and len(swapped):
                        plan_back()

                idx_mate(q).start()
                plan_block(q)

    def learn_leaf(s):
        for q, ok in ((pos - s, pos - s >= 0), (pos + s, pos + s < line))[:1 if s == 0 else 2]:
            @pl.when(ok)
            def _(q=q):
                idx_from_mate(q).wait_recv()
                plan_leaf(q)

    def arrive(s, c, tail=False):
        for q, ok, rightward in meets(s, c, tail):
            @pl.when(ok)
            def _(q=q, rightward=rightward):
                step = to_right if rightward else to_left
                step(q, c).wait_recv()

                @pl.when(pos < last if rightward else pos > 0)
                def _():
                    if not (s == last - 1 and c in swapped):
                        step(q, c).start()
                    if s == last - 1 and c == kept[-1]:
                        for n in late:
                            step(pos, n).start()

                if not (tail and c in crossed):
                    give_leaf(q, c)
                if s == last - 1 and c == chunks - 1 and len(held):
                    @pl.when(pos < last if rightward else pos > 0)
                    def _():
                        for n in held:
                            give_leaf(pos, n)

    def use(s, c, tail=False):
        for q, ok, rightward in meets(s, c, tail):
            @pl.when(ok)
            def _(q=q, rightward=rightward):
                use_block(q, c)
                closes(s, c, tail, done_block, q)
                if s == last - 1 and c in swapped:
                    @pl.when(pos < last if rightward else pos > 0)
                    def _():
                        back_arrival(c).wait_recv()
                        for b in range(2):
                            acc_r[b] += gathered(c, back[c][b], xb[c][q], tgt_r[b], tok_dev)
                        if c == swapped[-1]:
                            rst_r[...] = acc_r[...]
                            back_reply().start()
                            for n in crossed:
                                near_arrival(n).wait_recv()
                                acc_n[...] += gathered(n, back_n[n][...], xb[n][pos], tgt_n[...], tok_dev)

    def take(s, c, tail=False):
        if s == 0:
            if len(held) and (c in held or c == chunks - 1):
                if c not in held:
                    use_leaf(pos, c)

                @pl.when(near_end if tail else jnp.logical_not(near_end))
                def _():
                    if c in held:
                        use_leaf(pos, c)
                    if c == (held[-1] if tail else chunks - 1):
                        done_leaf(pos)
            else:
                use_leaf(pos, c)
                if c == chunks - 1:
                    done_leaf(pos)
            return
        for q, ok, _ in meets(s, c, tail):
            @pl.when(ok)
            def _(q=q):
                use_leaf(q, c)
                closes(s, c, tail, done_leaf, q)

    def settle(s, c):
        if c == 0:
            learn_leaf(s)
        take(s, c)

    def pass_rows(c):
        @pl.when(at_end)
        def _():
            if c in swapped:
                hop_rows(c).wait_recv()
                send_back(1, c).start()
            if c in crossed and c not in direct:
                hop_near(c).wait_recv()
                send_near(c).start()

    def sort_step(c):
        sort_rows(c)
        if c in swapped or c in crossed:
            @pl.when(at_end)
            def _():
                if c in swapped:
                    hop_rows(c).start()
                    send_back(0, c).start()
                if c in direct:
                    send_near(c).start()
                elif c in crossed:
                    hop_near(c).start()
        use_block(pos, c)
        if c == chunks - 1:
            rbuf[me] = acc_x[pos]

    part = tok_in.shape[1] // dp

    def tk_copy(s):
        return remote(tks.at[dp_peer(s)], tkr.at[md], s_tk, r_tk, (me, dp_peer(s)))

    def tk_all():
        return remote(tks.at[pl.ds(0, dp - 1)], tkr.at[pl.ds(0, dp - 1)], s_tk, r_tk, (me, dp_peer(1)))

    def sd_copy(s):
        return remote(st_dp.at[md], st_dp.at[md], s_sd, r_sd, (me, dp_peer(s)))

    def sd_all():
        return remote(st_dp.at[pl.ds(0, dp - 1)], st_dp.at[pl.ds(0, dp - 1)], s_sd, r_sd, (me, dp_peer(1)))

    def route():
        for copy in small:
            copy.wait()
        idx = idx_all[me]
        named = jnp.zeros((experts, tok_dev), F32)
        for k in range(chosen):
            named = named + jnp.where(idx[k:k + 1, :] == expert_row, 1.0, 0.0)
        logits = dot_nt(wt_v[...], tok_v[...]) + upright(bias_v[...])
        top = jnp.max(logits, axis=0, keepdims=True)
        power = jnp.exp(logits - top)
        prob = power / jnp.sum(power, axis=0, keepdims=True)
        logit_v[...] = logits
        prob_v[...] = prob
        named_v[...] = named
        ones = jnp.ones((8, tok_dev), F32)
        count_row = dot_nt(ones, named, lax.Precision.HIGHEST)
        prob_row = dot_nt(ones, prob, lax.Precision.HIGHEST)
        stat_row = lax.broadcasted_iota(jnp.int32, (8, experts), 0)
        st_dp[md] = jnp.where(stat_row == 0, count_row, prob_row)
        for s in range(1, dp):
            sd_copy(s).start()

    def share_tokens():
        for d in range(dp):
            tks[d] = tok_v[:, d * part:(d + 1) * part]
        for s in range(1, dp):
            tk_copy(s).start()
        tkr[md] = tks[md]

    def share_stats():
        sd_all().wait_recv()
        total = st_dp[0]
        for d in range(1, dp):
            total = total + st_dp[d]
        st_ep[me] = total
        loop_ep(lambda s: se_copy(s).start())

    plan_block(pos)
    for c in every:
        if c in held:
            @pl.when(jnp.logical_not(near_end))
            def _():
                give_leaf(pos, c)
        else:
            give_leaf(pos, c)
    rows_copy.wait()
    for c in every:
        if c == max(chunks - 2, 0):
            learn(1)
            arrive(1, 0)
        sort_step(c)
        if c < last:
            hear_ready(c)
    for n in range(chunks, last):
        hear_ready(n)
    steps = [(0, c) for c in every] + [(s, c) for s in range(1, line) for c in every]
    taken, tails = 0, []
    for n, (s, c) in enumerate(steps):
        if s == last and c in swapped:
            break
        if s > 0:
            if c == 0:
                if s > 1:
                    learn(s)
            if (s, c) != (1, 0):
                arrive(s, c)
            use(s, c)
            if (s, c) == (2, 0):
                for n in every:
                    if n in swapped or n in crossed:
                        pass_rows(n)
            if (s, c) == (1, 1 if chunks > 1 else 0):
                route()
                share_tokens()
            if (s, c) == (1, chunks - 1):
                share_stats()
            while taken <= n - LAG:
                settle(*steps[taken])
                taken += 1
    for m, c in enumerate(late):
        if m == 0 and taken < len(steps):
            settle(*steps[taken])
            taken += 1
        arrive(1, c, True)
        use(1, c, True)
        if m == 0:
            while taken < len(steps) and not (steps[taken][0] == last and steps[taken][1] in swapped):
                settle(*steps[taken])
                taken += 1
        if c not in crossed:
            tails.append(c)
    for step in steps[taken:]:
        settle(*step)
    for c in held:
        take(0, c, True)
    for c in tails:
        take(1, c, True)
    se_all().wait_recv()
    stats = lax.fori_loop(1, ep, lambda j, acc: acc + st_ep[j], st_ep[0])
    share = stats[0:1, :] / (token_total * chosen)
    mean = stats[1:2, :] / token_total
    loss_v[...] = experts * jnp.sum(share * mean, axis=1, keepdims=True)
    loss_copy = pltpu.make_async_copy(loss_v, loss_out, s_out)
    loss_copy.start()
    push_row = scale_v[...] * experts * share
    push = upright(push_row)
    prob = prob_v[...]
    spread = prob * (push - jnp.sum(prob * push, axis=0, keepdims=True))
    named = named_v[...]
    logits = logit_v[...]
    high = jnp.max(jnp.where(named > 0.5, logits, -jnp.inf), axis=0, keepdims=True)
    mix = jnp.where(named > 0.5, jnp.exp(jnp.minimum(logits - high, 0.0)), 0.0)
    mix = mix / jnp.sum(mix, axis=0, keepdims=True)

    remote(rst.at[pl.ds(0, ep - 1)], rbuf.at[pl.ds(0, ep - 1)], s_rep, r_rep, ep_id(mate)).wait_recv()
    if len(swapped):
        @pl.when(at_end)
        def _():
            back_reply_arrival().wait_recv()
            for b in range(2):
                rbuf[far * 2 + b] += rbuf_r[b]

        @pl.when(near_end)
        def _():
            rbuf[end * 2 + 1 - side] += acc_n[...]
    dots = jnp.concatenate([rbuf[j, 0:exp_dev, :] for j in range(ep)], axis=0)
    sel = mix * (dots - jnp.sum(mix * dots, axis=0, keepdims=True))
    grad = (spread + sel).astype(BF16)
    lgd[md] = grad

    def lg_copy(s):
        return remote(lgd.at[md], lgd.at[md], s_lg, r_lg, (me, dp_peer(s)))

    def lg_all():
        return remote(lgd.at[pl.ds(0, dp - 1)], lgd.at[pl.ds(0, dp - 1)], s_lg, r_lg, (me, dp_peer(1)))

    for s in range(1, dp):
        lg_copy(s).start()
    for c in every:
        at = slice(starts[c], starts[c] + widths[c])
        tg_out[:, at] = lax.dot_general(
            grad, wt_v[:, at], (((0,), (0,)), ((), ())), preferred_element_type=F32
        ).astype(BF16)
    tk_all().wait_recv()
    lg_all().wait_recv()
    term = dot_nn(lgd[0], tkr[0])
    for d in range(1, dp):
        term = term + dot_nn(lgd[d], tkr[d])
    for j in range(ep):
        ws[j] = term[j * exp_dev:(j + 1) * exp_dev, :]
    wr[me] = ws[me]

    def w_copy(s_):
        return remote(ws.at[ep_peer(s_)], wr.at[me], s_w, r_w, ep_id(ep_peer(s_)))

    def w_all():
        return remote(ws.at[pl.ds(0, ep - 1)], wr.at[pl.ds(0, ep - 1)], s_w, r_w, ep_id(mate))

    loop_ep(lambda s_: w_copy(s_).start())

    def sent(ref, sem, count):
        for n in range(1, line + 1):
            @pl.when(count == n)
            def _(n=n):
                piece = ref.at[pl.ds(0, n)]
                remote(piece, piece, sem, sem, ep_id(mate)).wait_send()

    ups = jnp.where(pos < last, pos + 1, 0)
    downs = jnp.where(pos > 0, line - pos, 0)
    sent(idx_all, s_idx.at[0], ups)
    sent(idx_all, s_idx.at[1], downs)
    sent(idx_all, s_idx.at[2], line)
    se_all().wait_send()
    for c in every:
        short = 1 if c in swapped else 0
        sent(xb[c], s_right.at[c], ups - jnp.where(pos == last - 1, short, 0))
        sent(xb[c], s_left.at[c], downs - jnp.where(pos == 1, short, 0))
        skipped = short + (1 if c in crossed else 0)
        sent(lsend[c], s_leaf.at[c], line - jnp.where(at_end, skipped, 0))
    if len(swapped):
        @pl.when(at_end)
        def _():
            for c in swapped:
                piece = rows_v[c].at[pl.ds(0, 3)]
                sem = s_back.at[swapped.index(c)]
                remote(piece, piece, sem, sem, ep_id(mate)).wait_send()
            for n, c in enumerate(crossed):
                piece = rows_v[c].at[pl.ds(0, 1 if c in direct else 2)]
                remote(piece, piece, s_near.at[n], s_near.at[n], ep_id(mate)).wait_send()

        @pl.when(near_end)
        def _():
            back_reply().wait_send()
    remote(rst.at[pl.ds(0, ep - 1)], rbuf.at[pl.ds(0, ep - 1)], s_rep, r_rep, ep_id(mate)).wait_send()
    sd_all().wait_send()
    tk_all().wait_send()
    lg_all().wait_send()
    loss_copy.wait()
    w_all().wait_recv()
    out = lax.fori_loop(1, ep, lambda j, acc: acc + wr[j], wr[0])
    wg_out[...] = out / math.sqrt(token_total)
    w_all().wait_send()


def finish(tg_in, wg_in, tg_out, wg_out, sems):
    copies = [pltpu.make_async_copy(tg_in, tg_out, sems.at[0]), pltpu.make_async_copy(wg_in, wg_out, sems.at[1])]
    for copy in copies:
        copy.start()
    for copy in copies:
        copy.wait()


def cut(width):
    if width <= 3 * CHUNK + CHUNK // 2 or width > 4 * CHUNK:
        widths = tuple(min(CHUNK, width - s) for s in range(0, width, CHUNK))
        return widths, tuple(sum(widths[:c]) for c in range(len(widths))), (), (), (), (), ()
    half = CHUNK // 2
    rest = width - 3 * CHUNK - half
    return (CHUNK, rest, half, CHUNK, CHUNK), (0, width - rest, CHUNK, CHUNK + half, 2 * CHUNK + half), (2, 3, 4), (4, 2, 1), (2, 1), (2,), (3,)


def on_device(tokens, out_grad, indices, expert_rows, router_weight, router_bias, balance_scale):
    tok_dev, width = tokens.shape
    chosen = indices.shape[1]
    experts = router_weight.shape[1]
    exp_dev, cap = expert_rows.shape[1], expert_rows.shape[3]
    ep = lax.axis_size("ep")
    dp = lax.axis_size("dp")
    line = ep // 2
    packed = -(-min(tok_dev, (exp_dev - 1) * cap) // 16) * 16
    widths, starts, swapped, late, crossed, direct, held = cut(width)
    chunks = len(widths)
    if line < 4:
        swapped, late, crossed, direct, held = (), (), (), (), ()
    part = width // dp
    rows_t = jnp.transpose(expert_rows[0], (0, 2, 1, 3)).reshape(exp_dev, cap * ep, width)
    hbm = pl.BlockSpec(memory_space=pl.ANY)
    vmem = pl.BlockSpec(memory_space=pltpu.VMEM)
    dma = pltpu.SemaphoreType.DMA
    height = -(-exp_dev * cap // 16) * 16
    folded = tuple(c for c in late if widths[c] == 192 and tok_dev % 16 == 0)

    def room(*shape):
        rows = shape[-1]
        return [
            pltpu.VMEM(shape[:-1] + ((-(-rows * 3 // 32) * 16, 128) if c in folded else (rows, w)), BF16)
            for c, w in enumerate(widths)
        ]

    cfg = (ep, dp, tok_dev, chosen, experts, exp_dev, cap, packed, widths, starts, swapped, late, crossed, direct, held, folded, tok_dev * ep * dp)
    scratch = room(line, tok_dev) + room(line, packed) + room(line, packed) + room(ep, height)
    scratch += room(2, height) + room(height) + room(height) + room(height)
    scratch += [
        pltpu.VMEM((tok_dev, width), BF16),
        pltpu.VMEM((experts, width), BF16),
        pltpu.VMEM((1, experts), F32),
        pltpu.VMEM((1, 1), F32),
        dma((5,)),
        pltpu.VMEM((1, 1), F32),
        dma,
        pltpu.VMEM((tok_dev, 192), BF16),
        pltpu.VMEM((exp_dev, cap * ep, width), BF16),
        pltpu.VMEM((exp_dev, ep * (-(-cap // 8) * 8), max(widths)), F32),
        pltpu.VMEM((2, 8, tok_dev), F32),
        pltpu.VMEM((2, 8, tok_dev), F32),
        pltpu.VMEM((2, 8, tok_dev), F32),
        pltpu.VMEM((2, 8, tok_dev), F32),
        *[dma((max(len(swapped), 1),))] * 3, *[dma((max(len(crossed), 1),))] * 3, dma, dma,
        pltpu.VMEM((8, tok_dev), F32),
        pltpu.VMEM((8, tok_dev), F32),
        pltpu.VMEM((ep, chosen, tok_dev), jnp.int32),
        pltpu.VMEM((line, packed, tok_dev), BF16),
        pltpu.VMEM((line, packed, tok_dev), BF16),
        pltpu.VMEM((line, 8, tok_dev), F32),
        pltpu.VMEM((line, 8, packed), F32),
        pltpu.VMEM((line, 8, tok_dev), F32),
        pltpu.VMEM((line, 8, packed), F32),
        pltpu.VMEM((ep, 8, tok_dev), F32),
        pltpu.VMEM((ep, 8, tok_dev), F32),
        pltpu.VMEM((dp, tok_dev, part), BF16),
        pltpu.VMEM((dp, tok_dev, part), BF16),
        pltpu.VMEM((experts, tok_dev), F32),
        pltpu.VMEM((experts, tok_dev), F32),
        pltpu.VMEM((experts, tok_dev), F32),
        pltpu.VMEM((dp, 8, experts), F32),
        pltpu.VMEM((ep, 8, experts), F32),
        pltpu.VMEM((dp, experts, tok_dev), BF16),
        pltpu.VMEM((ep, exp_dev, part), F32),
        pltpu.VMEM((ep, exp_dev, part), F32),
        dma, dma((chunks,)), dma((3,)), dma((ep,)),
        dma((chunks,)), dma((chunks,)), dma((max(line - 1, 1), chunks)),
        dma((chunks,)), dma((line, chunks)), dma, dma,
        dma, dma, dma, dma, dma, dma, pltpu.SemaphoreType.REGULAR((max(line - 1, 1),)),
        dma, dma, dma, dma,
    ]
    token_grad, wg, loss = pl.pallas_call(
        functools.partial(kernel, cfg),
        name="router_backward",
        out_shape=(
            pltpu.VMEM((tok_dev, width), BF16),
            pltpu.VMEM((exp_dev, part), F32),
            jax.ShapeDtypeStruct((1, 1), F32),
        ),
        in_specs=[hbm] * 7,
        out_specs=(vmem, vmem, hbm),
        scratch_shapes=scratch,
        compiler_params=pltpu.CompilerParams(
            collective_id=0, has_side_effects=True, vmem_limit_bytes=56 * 1024 * 1024
        ),
    )(indices.T, out_grad, rows_t, tokens, router_weight.T, router_bias.reshape(1, experts), balance_scale.reshape(1, 1))
    token_grad, wg = pl.pallas_call(
        finish,
        name="write_out",
        out_shape=(
            jax.ShapeDtypeStruct(token_grad.shape, token_grad.dtype),
            jax.ShapeDtypeStruct(wg.shape, wg.dtype),
        ),
        in_specs=[vmem, vmem],
        out_specs=(hbm, hbm),
        scratch_shapes=[dma((2,))],
    )(*(pltpu.with_memory_space_constraint(x, pltpu.VMEM) for x in (token_grad, wg)))
    return (token_grad, wg.T, loss.reshape(1))


def solution(mesh):
    placed = (
        P(("ep", "dp"), None),
        P(("ep", "dp"), None),
        P(("ep", "dp"), None),
        P("dp", "ep", None, None, None),
        P(),
        P(),
        P(),
    )
    return jax.shard_map(
        on_device,
        mesh=mesh,
        in_specs=placed,
        out_specs=(P(("ep", "dp"), None), P("dp", "ep"), P()),
        check_vma=False,
    )
```

```python
import functools
import math

import jax
import jax.numpy as jnp
from jax import lax
from jax.experimental import pallas as pl
from jax.experimental.pallas import tpu as pltpu
from jax.sharding import PartitionSpec as P

MESH = pl.DeviceIdType.MESH
F32 = jnp.float32
BF16 = jnp.bfloat16
CHUNK = 768
LAG = 4


def dot_nt(x, y, precision=None):
    return lax.dot_general(
        x, y, (((1,), (1,)), ((), ())), preferred_element_type=F32, precision=precision
    )


def dot_nn(x, y, precision=None):
    return lax.dot_general(
        x, y, (((1,), (0,)), ((), ())), preferred_element_type=F32, precision=precision
    )


def fold(left, right):
    half = right.shape[0] // 2
    pieces = [left, jnp.concatenate([right[0:half], right[half:]], axis=1)]
    short = -3 * half % 16
    if short:
        pieces.append(jnp.zeros((short, 128), F32))
    return jnp.concatenate(pieces, axis=0)


def unfold(x, rows):
    low = x[rows:, :].astype(F32)[0:rows // 2]
    return x[0:rows], jnp.concatenate([low[:, 0:64], low[:, 64:128]], axis=0).astype(BF16)


def kernel(cfg, *refs):
    (ep, dp, tok_dev, chosen, experts, exp_dev, cap, packed, widths, starts, swapped, late, crossed, direct, held, folded, token_total) = cfg
    line = ep // 2
    last = line - 1
    chunks = len(widths)
    every = range(chunks)
    kept = [c for c in every if c not in swapped]
    (idx_in, grad_in, rows_in, tok_in, wt_in, bias_in, scale_in, tg_out, wg_out, loss_out) = refs[:10]
    refs = refs[10:]
    hop = refs[5 * chunks:6 * chunks]
    hop_n = refs[6 * chunks:7 * chunks]
    back_n = refs[7 * chunks:8 * chunks]
    xb = refs[:chunks]
    lsend = refs[chunks:2 * chunks]
    lrecv = refs[2 * chunks:3 * chunks]
    rows_v = refs[3 * chunks:4 * chunks]
    back = refs[4 * chunks:5 * chunks]
    (tok_v, wt_v, bias_v, scale_v, s_in, loss_v, s_out, stage,
     rows_raw, piled, tgt_r, acc_r, rst_r, rbuf_r, s_back, r_back, r_hop, s_near, r_hop_n, r_back_n, s_rr, r_rr, tgt_n, acc_n,
     idx_all, pin, pout, tgt_x, tgt_p, acc_x, acc_p, rst, rbuf, tks, tkr, mp, nbuf, st_dp, st_ep, lgd, ws, wr,
     s_rows, s_own, s_idx, r_idx, s_right, s_left, r_x, s_leaf, r_leaf, s_rep, r_rep,
     s_tk, r_tk, s_sd, r_sd, s_se, r_se, s_ready, s_mp, r_mp, s_nb, r_nb, s_w, r_w) = refs[8 * chunks:]
    me = lax.axis_index("ep")
    md = lax.axis_index("dp")
    pos = me // 2
    side = lax.rem(me, 2)
    mate = pos * 2 + 1 - side
    at_end = jnp.logical_or(pos == 0, pos == last)
    near_end = jnp.logical_or(pos == 1, pos == last - 1)
    end = jnp.where(pos * 2 < line, 0, last)
    near = jnp.where(pos * 2 < line, 1, last - 1)
    far = last - end

    def ep_id(other):
        return (other, md)

    def remote(src, dst, s, r, dev):
        return pltpu.make_async_remote_copy(
            src_ref=src, dst_ref=dst, send_sem=s, recv_sem=r, device_id=dev, device_id_type=MESH
        )

    def ep_peer(s):
        return lax.rem(me + s, ep)

    def dp_peer(s):
        return lax.rem(md + s, dp)

    barrier = pltpu.get_barrier_semaphore()

    def greet(dev):
        pl.semaphore_signal(barrier, inc=1, device_id=dev, device_id_type=MESH)

    @pl.when(pos < last)
    def _():
        greet(ep_id(me + 2))

    @pl.when(pos > 0)
    def _():
        greet(ep_id(me - 2))

    greet(ep_id(mate))
    for s in range(1, dp):
        greet((me, dp_peer(s)))

    idx_here = pltpu.make_async_copy(idx_in, idx_all.at[me], s_in.at[0])
    own = [
        pltpu.make_async_copy(
            grad_in.at[:, pl.ds(starts[c], widths[c])], stage if c in folded else xb[c].at[pos], s_own.at[c]
        )
        for c in every
    ]
    rows_copy = pltpu.make_async_copy(rows_in, rows_raw, s_rows)
    small = [
        pltpu.make_async_copy(tok_in, tok_v, s_in.at[1]),
        pltpu.make_async_copy(wt_in, wt_v, s_in.at[2]),
        pltpu.make_async_copy(bias_in, bias_v, s_in.at[3]),
        pltpu.make_async_copy(scale_in, scale_v, s_in.at[4]),
    ]
    idx_here.start()
    for copy in own:
        copy.start()
    rows_copy.start()
    for copy in small:
        copy.start()
    pl.semaphore_wait(
        barrier, dp + (pos < last).astype(jnp.int32) + (pos > 0).astype(jnp.int32)
    )

    def idx_copy(q, way, dev):
        at = q * 2 + side
        return remote(idx_all.at[at], idx_all.at[at], s_idx.at[way], r_idx.at[at], ep_id(dev))

    def idx_right(q):
        return idx_copy(q, 0, me + 2)

    def idx_left(q):
        return idx_copy(q, 1, me - 2)

    def idx_mate(q):
        return idx_copy(q, 2, mate)

    def idx_from_mate(q):
        at = q * 2 + 1 - side
        return remote(idx_all.at[at], idx_all.at[at], s_idx.at[2], r_idx.at[at], ep_id(mate))

    def loop_ep(fn):
        def body(s, carry):
            fn(s)
            return carry
        lax.fori_loop(1, ep, body, 0)

    def to_right(q, c):
        return remote(xb[c].at[q], xb[c].at[q], s_right.at[c], r_x.at[q, c], ep_id(me + 2))

    def to_left(q, c):
        return remote(xb[c].at[q], xb[c].at[q], s_left.at[c], r_x.at[q - 1, c], ep_id(me - 2))

    def leaf(q, c):
        return remote(lsend[c].at[q], lrecv[c].at[q], s_leaf.at[c], r_leaf.at[q, c], ep_id(mate))

    def hop_rows(c):
        return remote(rows_v[c].at[far * 2 + 1 - side], hop[c], s_back.at[swapped.index(c)], r_hop.at[swapped.index(c)], ep_id(mate))

    def send_back(b, c):
        src = rows_v[c].at[far * 2 + side] if b == 0 else hop[c]
        at = side if b == 0 else 1 - side
        return remote(src, back[c].at[at], s_back.at[swapped.index(c)], r_back.at[swapped.index(c)], ep_id(near * 2 + side))

    def back_arrival(c):
        return remote(back[c], back[c], s_back.at[swapped.index(c)], r_back.at[swapped.index(c)], ep_id(end * 2 + side))

    def hop_near(c):
        n = crossed.index(c)
        return remote(rows_v[c].at[near * 2 + 1 - side], hop_n[c], s_near.at[n], r_hop_n.at[n], ep_id(mate))

    def send_near(c):
        n = crossed.index(c)
        if c in direct:
            return remote(rows_v[c].at[near * 2 + 1 - side], back_n[c], s_near.at[n], r_back_n.at[n], ep_id(near * 2 + 1 - side))
        return remote(hop_n[c], back_n[c], s_near.at[n], r_back_n.at[n], ep_id(near * 2 + side))

    def near_arrival(c):
        n = crossed.index(c)
        return remote(back_n[c], back_n[c], s_near.at[n], r_back_n.at[n], ep_id(end * 2 + side))

    def back_reply(d):
        return remote(rst_r, rbuf_r.at[md], s_rr, r_rr, (far * 2 + side, d))

    def back_replies():
        return remote(rbuf_r, rbuf_r, s_rr, r_rr, ep_id((last - near) * 2 + side))

    def reply(j, d):
        return remote(rst.at[j], rbuf.at[md * ep + me], s_rep, r_rep, (j, d))

    def replies():
        piece = rbuf.at[pl.ds(0, ep * dp - 1)]
        return remote(piece, piece, s_rep, r_rep, ep_id(mate))

    def near_share(s):
        return remote(nbuf.at[md], nbuf.at[md], s_nb, r_nb, (me, dp_peer(s)))

    def near_shares():
        piece = nbuf.at[pl.ds(0, dp - 1)]
        return remote(piece, piece, s_nb, r_nb, (me, dp_peer(1)))

    def mp_copy(s):
        return remote(mp.at[md], mp.at[md], s_mp, r_mp, (me, dp_peer(s)))

    def mp_all():
        piece = mp.at[pl.ds(0, dp - 1)]
        return remote(piece, piece, s_mp, r_mp, (me, dp_peer(1)))

    def se_copy(s):
        return remote(st_ep.at[me], st_ep.at[me], s_se, r_se, ep_id(ep_peer(s)))

    def se_all():
        return remote(st_ep.at[pl.ds(0, ep - 1)], st_ep.at[pl.ds(0, ep - 1)], s_se, r_se, ep_id(mate))

    def say_ready(n):
        def tell(dev):
            pl.semaphore_signal(s_ready.at[n], inc=1, device_id=ep_id(dev), device_id_type=MESH)

        @pl.when(pos < last)
        def _():
            tell(me + 2)

        @pl.when(pos > 0)
        def _():
            tell(me - 2)

        tell(mate)

    def hear_ready(n):
        pl.semaphore_wait(s_ready.at[n], 1 + (pos < last).astype(jnp.int32) + (pos > 0).astype(jnp.int32))
        if n + 1 < last:
            say_ready(n + 1)

    if last > 0:
        say_ready(0)
    for copy in own:
        copy.wait()
    idx_here.wait()

    @pl.when(pos < last)
    def _():
        idx_right(pos).start()

    @pl.when(pos > 0)
    def _():
        idx_left(pos).start()

    idx_mate(pos).start()
    for c in every:
        if c in folded:
            xb[c][pos] = fold(stage[:, 0:128].astype(F32), stage[:, 128:192].astype(F32)).astype(BF16)

        @pl.when(pos < last - (c in late))
        def _():
            to_right(pos, c).start()

        @pl.when(pos > 0 + (c in late))
        def _():
            to_left(pos, c).start()

    expert_row = lax.broadcasted_iota(jnp.int32, (experts, tok_dev), 0)
    eye_r = lax.broadcasted_iota(jnp.int32, (experts, experts), 0)
    eye_c = lax.broadcasted_iota(jnp.int32, (experts, experts), 1)
    t_from = lax.broadcasted_iota(jnp.int32, (tok_dev, tok_dev), 0)
    t_to = lax.broadcasted_iota(jnp.int32, (tok_dev, tok_dev), 1)
    upper = jnp.where(t_from < t_to, 1.0, 0.0).astype(BF16)
    row8 = lax.broadcasted_iota(jnp.int32, (8, tok_dev), 0)
    slot_p = lax.broadcasted_iota(jnp.int32, (packed, tok_dev), 0).astype(F32)

    def upright(line_of):
        return jnp.sum(jnp.where(eye_r == eye_c, line_of, 0.0), axis=1, keepdims=True)

    def plan(table, group):
        who = jnp.where(row8 < exp_dev, group * exp_dev + row8, -2)
        hit = jnp.zeros((8, tok_dev), F32)
        for k in range(chosen):
            hit = hit + jnp.where(table[k:k + 1, :] == who, 1.0, 0.0)
        need = jnp.max(hit, axis=0, keepdims=True)
        stack = jnp.where(row8 == exp_dev, need, hit)
        before = dot_nn(stack.astype(BF16), upper)
        place = jnp.where(need > 0.5, before[exp_dev:exp_dev + 1, :], -1.0)
        target = jnp.where(hit > 0.5, before, -1.0)
        pack = jnp.where(slot_p == place, 1.0, 0.0).astype(BF16)
        return target, pack

    def plan_block(q):
        table = idx_all[q * 2 + side]
        _, pack = plan(table, mate)
        pout[q] = pack
        target, _ = plan(table, me)
        tgt_x[q] = target
        acc_x[q] = jnp.zeros((8, tok_dev), F32)

    def plan_leaf(q):
        target, pack = plan(idx_all[q * 2 + 1 - side], me)
        pin[q] = pack
        tgt_p[q] = dot_nt((target + 1.0).astype(BF16), pack) - 1.0
        acc_p[q] = jnp.zeros((8, packed), F32)

    def plan_back():
        for b in range(2):
            tgt_r[b], _ = plan(idx_all[far * 2 + side], end * 2 + b)
            acc_r[b] = jnp.zeros((8, tok_dev), F32)
        tgt_n[...], _ = plan(idx_all[me], end * 2 + 1 - side)
        acc_n[...] = jnp.zeros((8, tok_dev), F32)

    deep = piled.shape[1] // ep
    slot_r = lax.broadcasted_iota(jnp.int32, (deep, cap * ep), 0)
    lies = lax.broadcasted_iota(jnp.int32, (deep, cap * ep), 1)
    spare = -exp_dev * cap % 16

    def sort_rows(c):
        w = widths[c]
        order = jnp.concatenate(
            [jnp.where(jnp.logical_and(lies == slot_r * ep + j, slot_r < cap), 1.0, 0.0) for j in range(ep)], axis=0
        ).astype(BF16)
        for e in range(exp_dev):
            piled[e, :, 0:w] = dot_nn(order, rows_raw[e, :, starts[c]:starts[c] + w])

        def put(j, carry):
            at = pl.ds(pl.multiple_of(j * deep, 8), deep)
            pieces = [piled[e, at, 0:w][0:cap, :] for e in range(exp_dev)]
            if spare:
                pieces.append(jnp.zeros((spare, w), F32))
            block = jnp.concatenate(pieces, axis=0)
            if c in folded:
                block = fold(block[:, 0:128], block[:, 128:192])
            rows_v[c][j] = block.astype(BF16)
            return carry

        lax.fori_loop(0, ep, put, 0)

    def all_dots(c, table, block, count):
        if c not in folded:
            return dot_nt(table, block)
        (table_l, table_r), (block_l, block_r) = unfold(table, exp_dev * cap + spare), unfold(block, count)
        return dot_nt(table_l, block_l) + dot_nt(table_r, block_r)

    def gathered(c, table, block, target, count):
        dots = all_dots(c, table, block, count)
        height = dots.shape[0]
        slot = lax.broadcasted_iota(jnp.int32, (height, count), 0).astype(F32)
        row = lax.broadcasted_iota(jnp.int32, (8, count), 0)
        out = jnp.zeros((8, count), F32)
        for e in range(exp_dev):
            want = jnp.where(target[e:e + 1, :] >= 0.0, target[e:e + 1, :] + e * cap, -1.0)
            one = jnp.sum(jnp.where(slot == want, dots, 0.0), axis=0, keepdims=True)
            out = jnp.where(row == e, one, out)
        return out

    def give_leaf(q, c):
        if c in folded:
            left, right = unfold(xb[c][q], tok_dev)
            lsend[c][q] = fold(dot_nn(pout[q], left), dot_nn(pout[q], right)).astype(BF16)
        else:
            lsend[c][q] = dot_nn(pout[q], xb[c][q]).astype(BF16)
        leaf(q, c).start()

    def use_block(q, c):
        acc_x[q] += gathered(c, rows_v[c][q * 2 + side], xb[c][q], tgt_x[q], tok_dev)

    def use_leaf(q, c):
        leaf(q, c).wait_recv()
        acc_p[q] += gathered(c, rows_v[c][q * 2 + 1 - side], lrecv[c][q], tgt_p[q], packed)

    def answer(j, value):
        rst[j] = value[0:exp_dev]
        for d in range(dp):
            reply(j, d).start()

    def done_block(q):
        answer(q * 2 + side, acc_x[q])

    def done_leaf(q):
        answer(q * 2 + 1 - side, dot_nn(acc_p[q], pin[q].astype(F32), lax.Precision.HIGHEST))

    def meets(s, c, tail):
        left, right = pos - s >= 0, pos + s < line
        if s == last and c in swapped:
            return ()
        if s == 1 and c in late:
            inner = at_end if tail else jnp.logical_not(at_end)
            left, right = jnp.logical_and(left, inner), jnp.logical_and(right, inner)
        return ((pos - s, left, True), (pos + s, right, False))

    def closes(s, c, tail, finish, q):
        if s == 1 and len(late):
            ends = [n for n in late if finish is done_block or n not in crossed]
            if tail:
                if c == ends[-1]:
                    finish(q)
            elif c == chunks - 1:
                @pl.when(jnp.logical_not(at_end))
                def _():
                    finish(q)
        elif c == (kept[-1] if s == last else chunks - 1):
            finish(q)

    def learn(s):
        for q, ok, rightward in ((pos - s, pos - s >= 0, True), (pos + s, pos + s < line, False)):
            @pl.when(ok)
            def _(q=q, rightward=rightward):
                step = idx_right if rightward else idx_left
                step(q).wait_recv()

                @pl.when(pos < last if rightward else pos > 0)
                def _():
                    step(q).start()
                    if s == last - 1 and len(swapped):
                        plan_back()

                idx_mate(q).start()
                plan_block(q)

    def learn_leaf(s):
        for q, ok in ((pos - s, pos - s >= 0), (pos + s, pos + s < line))[:1 if s == 0 else 2]:
            @pl.when(ok)
            def _(q=q):
                idx_from_mate(q).wait_recv()
                plan_leaf(q)

    def arrive(s, c, tail=False):
        for q, ok, rightward in meets(s, c, tail):
            @pl.when(ok)
            def _(q=q, rightward=rightward):
                step = to_right if rightward else to_left
                step(q, c).wait_recv()

                @pl.when(pos < last if rightward else pos > 0)
                def _():
                    if not (s == last - 1 and c in swapped):
                        step(q, c).start()
                    if s == last - 1 and c == kept[-1]:
                        for n in late:
                            step(pos, n).start()

                if not (tail and c in crossed):
                    give_leaf(q, c)
                if s == last - 1 and c == chunks - 1 and len(held):
                    @pl.when(pos < last if rightward else pos > 0)
                    def _():
                        for n in held:
                            give_leaf(pos, n)

    def use(s, c, tail=False):
        for q, ok, rightward in meets(s, c, tail):
            @pl.when(ok)
            def _(q=q, rightward=rightward):
                use_block(q, c)
                closes(s, c, tail, done_block, q)
                if s == last - 1 and c in swapped:
                    @pl.when(pos < last if rightward else pos > 0)
                    def _():
                        back_arrival(c).wait_recv()
                        for b in range(2):
                            acc_r[b] += gathered(c, back[c][b], xb[c][q], tgt_r[b], tok_dev)
                        if c == swapped[-1]:
                            rst_r[...] = acc_r[:, 0:exp_dev, :]
                            for d in range(dp):
                                back_reply(d).start()
                            for n in crossed:
                                near_arrival(n).wait_recv()
                                acc_n[...] += gathered(n, back_n[n][...], xb[n][pos], tgt_n[...], tok_dev)
                            nbuf[md] = acc_n[0:exp_dev]
                            for n in range(1, dp):
                                near_share(n).start()

    def take(s, c, tail=False):
        if s == 0:
            if len(held) and (c in held or c == chunks - 1):
                if c not in held:
                    use_leaf(pos, c)

                @pl.when(near_end if tail else jnp.logical_not(near_end))
                def _():
                    if c in held:
                        use_leaf(pos, c)
                    if c == (held[-1] if tail else chunks - 1):
                        done_leaf(pos)
            else:
                use_leaf(pos, c)
                if c == chunks - 1:
                    done_leaf(pos)
            return
        for q, ok, _ in meets(s, c, tail):
            @pl.when(ok)
            def _(q=q):
                use_leaf(q, c)
                closes(s, c, tail, done_leaf, q)

    def settle(s, c):
        if c == 0:
            learn_leaf(s)
        take(s, c)

    def pass_rows(c):
        @pl.when(at_end)
        def _():
            if c in swapped:
                hop_rows(c).wait_recv()
                send_back(1, c).start()
            if c in crossed and c not in direct:
                hop_near(c).wait_recv()
                send_near(c).start()

    def sort_step(c):
        sort_rows(c)
        if c in swapped or c in crossed:
            @pl.when(at_end)
            def _():
                if c in swapped:
                    hop_rows(c).start()
                    send_back(0, c).start()
                if c in direct:
                    send_near(c).start()
                elif c in crossed:
                    hop_near(c).start()
        use_block(pos, c)
        if c == chunks - 1:
            rst[me] = acc_x[pos][0:exp_dev]
            rbuf[md * ep + me] = acc_x[pos][0:exp_dev]
            for n in range(1, dp):
                reply(me, dp_peer(n)).start()

    part = tok_in.shape[1] // dp

    def tk_copy(s):
        return remote(tks.at[dp_peer(s)], tkr.at[md], s_tk, r_tk, (me, dp_peer(s)))

    def tk_all():
        return remote(tks.at[pl.ds(0, dp - 1)], tkr.at[pl.ds(0, dp - 1)], s_tk, r_tk, (me, dp_peer(1)))

    def sd_copy(s):
        return remote(st_dp.at[md], st_dp.at[md], s_sd, r_sd, (me, dp_peer(s)))

    def sd_all():
        return remote(st_dp.at[pl.ds(0, dp - 1)], st_dp.at[pl.ds(0, dp - 1)], s_sd, r_sd, (me, dp_peer(1)))

    def route():
        for copy in small:
            copy.wait()
        idx = idx_all[me]
        named = jnp.zeros((experts, tok_dev), F32)
        for k in range(chosen):
            named = named + jnp.where(idx[k:k + 1, :] == expert_row, 1.0, 0.0)
        logits = dot_nt(wt_v[...], tok_v[...]) + upright(bias_v[...])
        top = jnp.max(logits, axis=0, keepdims=True)
        power = jnp.exp(logits - top)
        prob = power / jnp.sum(power, axis=0, keepdims=True)
        high = jnp.max(jnp.where(named > 0.5, logits, -jnp.inf), axis=0, keepdims=True)
        mix = jnp.where(named > 0.5, jnp.exp(jnp.minimum(logits - high, 0.0)), 0.0)
        mp[md, 0] = mix / jnp.sum(mix, axis=0, keepdims=True)
        mp[md, 1] = prob
        ones = jnp.ones((8, tok_dev), F32)
        count_row = dot_nt(ones, named, lax.Precision.HIGHEST)
        prob_row = dot_nt(ones, prob, lax.Precision.HIGHEST)
        stat_row = lax.broadcasted_iota(jnp.int32, (8, experts), 0)
        st_dp[md] = jnp.where(stat_row == 0, count_row, prob_row)
        for s in range(1, dp):
            sd_copy(s).start()
        for s in range(1, dp):
            mp_copy(s).start()

    def share_tokens():
        for d in range(dp):
            tks[d] = tok_v[:, d * part:(d + 1) * part]
        for s in range(1, dp):
            tk_copy(s).start()
        tkr[md] = tks[md]

    def share_stats():
        sd_all().wait_recv()
        total = st_dp[0]
        for d in range(1, dp):
            total = total + st_dp[d]
        st_ep[me] = total
        loop_ep(lambda s: se_copy(s).start())

    plan_block(pos)
    for c in every:
        if c in held:
            @pl.when(jnp.logical_not(near_end))
            def _():
                give_leaf(pos, c)
        else:
            give_leaf(pos, c)
    rows_copy.wait()
    for c in every:
        if c == max(chunks - 2, 0):
            learn(1)
            arrive(1, 0)
        sort_step(c)
        if c < last:
            hear_ready(c)
    for n in range(chunks, last):
        hear_ready(n)
    steps = [(0, c) for c in every] + [(s, c) for s in range(1, line) for c in every]
    taken, tails = 0, []
    for n, (s, c) in enumerate(steps):
        if s == last and c in swapped:
            break
        if s > 0:
            if c == 0:
                if s > 1:
                    learn(s)
            if (s, c) != (1, 0):
                arrive(s, c)
            use(s, c)
            if (s, c) == (2, 0):
                for n in every:
                    if n in swapped or n in crossed:
                        pass_rows(n)
            if (s, c) == (1, 1 if chunks > 1 else 0):
                route()
                share_tokens()
            if (s, c) == (1, chunks - 1):
                share_stats()
            while taken <= n - LAG:
                settle(*steps[taken])
                taken += 1
    for m, c in enumerate(late):
        if m == 0 and taken < len(steps):
            settle(*steps[taken])
            taken += 1
        arrive(1, c, True)
        use(1, c, True)
        if m == 0:
            while taken < len(steps) and not (steps[taken][0] == last and steps[taken][1] in swapped):
                settle(*steps[taken])
                taken += 1
        if c not in crossed:
            tails.append(c)
    for step in steps[taken:]:
        settle(*step)
    for c in held:
        take(0, c, True)
    for c in tails:
        take(1, c, True)
    se_all().wait_recv()
    stats = lax.fori_loop(1, ep, lambda j, acc: acc + st_ep[j], st_ep[0])
    share = stats[0:1, :] / (token_total * chosen)
    mean = stats[1:2, :] / token_total
    loss_v[...] = experts * jnp.sum(share * mean, axis=1, keepdims=True)
    loss_copy = pltpu.make_async_copy(loss_v, loss_out, s_out)
    loss_copy.start()
    push_row = scale_v[...] * experts * share
    push = upright(push_row)
    mp_all().wait_recv()
    tk_all().wait_recv()
    spreads = []
    for d in range(dp):
        prob = mp[d, 1]
        spreads.append(prob * (push - jnp.sum(prob * push, axis=0, keepdims=True)))
    replies().wait_recv()
    if len(swapped):
        @pl.when(at_end)
        def _():
            back_replies().wait_recv()
            for d in range(dp):
                for b in range(2):
                    rbuf[d * ep + far * 2 + b] += rbuf_r[d, b]

        @pl.when(near_end)
        def _():
            near_shares().wait_recv()
            for d in range(dp):
                rbuf[d * ep + end * 2 + 1 - side] += nbuf[d]
    for d in range(dp):
        mix = mp[d, 0]
        dots = jnp.concatenate([rbuf[d * ep + j] for j in range(ep)], axis=0)
        sel = mix * (dots - jnp.sum(mix * dots, axis=0, keepdims=True))
        lgd[d] = (spreads[d] + sel).astype(BF16)
    term = dot_nn(lgd[0], tkr[0])
    for d in range(1, dp):
        term = term + dot_nn(lgd[d], tkr[d])
    for j in range(ep):
        ws[j] = term[j * exp_dev:(j + 1) * exp_dev, :]
    wr[me] = ws[me]

    def w_copy(s_):
        return remote(ws.at[ep_peer(s_)], wr.at[me], s_w, r_w, ep_id(ep_peer(s_)))

    def w_all():
        return remote(ws.at[pl.ds(0, ep - 1)], wr.at[pl.ds(0, ep - 1)], s_w, r_w, ep_id(mate))

    loop_ep(lambda s_: w_copy(s_).start())
    grad = lgd[md]
    for c in every:
        at = slice(starts[c], starts[c] + widths[c])
        tg_out[:, at] = lax.dot_general(
            grad, wt_v[:, at], (((0,), (0,)), ((), ())), preferred_element_type=F32
        ).astype(BF16)

    def sent(ref, sem, count):
        for n in range(1, line + 1):
            @pl.when(count == n)
            def _(n=n):
                piece = ref.at[pl.ds(0, n)]
                remote(piece, piece, sem, sem, ep_id(mate)).wait_send()

    ups = jnp.where(pos < last, pos + 1, 0)
    downs = jnp.where(pos > 0, line - pos, 0)
    sent(idx_all, s_idx.at[0], ups)
    sent(idx_all, s_idx.at[1], downs)
    sent(idx_all, s_idx.at[2], line)
    se_all().wait_send()
    for c in every:
        short = 1 if c in swapped else 0
        sent(xb[c], s_right.at[c], ups - jnp.where(pos == last - 1, short, 0))
        sent(xb[c], s_left.at[c], downs - jnp.where(pos == 1, short, 0))
        skipped = short + (1 if c in crossed else 0)
        sent(lsend[c], s_leaf.at[c], line - jnp.where(at_end, skipped, 0))
    if len(swapped):
        @pl.when(at_end)
        def _():
            for c in swapped:
                piece = rows_v[c].at[pl.ds(0, 3)]
                sem = s_back.at[swapped.index(c)]
                remote(piece, piece, sem, sem, ep_id(mate)).wait_send()
            for n, c in enumerate(crossed):
                piece = rows_v[c].at[pl.ds(0, 1 if c in direct else 2)]
                remote(piece, piece, s_near.at[n], s_near.at[n], ep_id(mate)).wait_send()

        @pl.when(near_end)
        def _():
            back_replies().wait_send()
            near_shares().wait_send()
    replies().wait_send()
    mp_all().wait_send()
    sd_all().wait_send()
    tk_all().wait_send()
    loss_copy.wait()
    w_all().wait_recv()
    out = lax.fori_loop(1, ep, lambda j, acc: acc + wr[j], wr[0])
    wg_out[...] = out / math.sqrt(token_total)
    w_all().wait_send()


def finish(tg_in, wg_in, tg_out, wg_out, sems):
    copies = [pltpu.make_async_copy(tg_in, tg_out, sems.at[0]), pltpu.make_async_copy(wg_in, wg_out, sems.at[1])]
    for copy in copies:
        copy.start()
    for copy in copies:
        copy.wait()


def cut(width):
    if width <= 3 * CHUNK + CHUNK // 2 or width > 4 * CHUNK:
        widths = tuple(min(CHUNK, width - s) for s in range(0, width, CHUNK))
        return widths, tuple(sum(widths[:c]) for c in range(len(widths))), (), (), (), (), ()
    half = CHUNK // 2
    rest = width - 3 * CHUNK - half
    return (CHUNK, rest, half, CHUNK, CHUNK), (0, width - rest, CHUNK, CHUNK + half, 2 * CHUNK + half), (2, 3, 4), (4, 2, 1), (2, 1), (2,), (3,)


def on_device(tokens, out_grad, indices, expert_rows, router_weight, router_bias, balance_scale):
    tok_dev, width = tokens.shape
    chosen = indices.shape[1]
    experts = router_weight.shape[1]
    exp_dev, cap = expert_rows.shape[1], expert_rows.shape[3]
    ep = lax.axis_size("ep")
    dp = lax.axis_size("dp")
    line = ep // 2
    packed = -(-min(tok_dev, (exp_dev - 1) * cap) // 16) * 16
    widths, starts, swapped, late, crossed, direct, held = cut(width)
    chunks = len(widths)
    if line < 4:
        swapped, late, crossed, direct, held = (), (), (), (), ()
    part = width // dp
    rows_t = jnp.transpose(expert_rows[0], (0, 2, 1, 3)).reshape(exp_dev, cap * ep, width)
    hbm = pl.BlockSpec(memory_space=pl.ANY)
    vmem = pl.BlockSpec(memory_space=pltpu.VMEM)
    dma = pltpu.SemaphoreType.DMA
    height = -(-exp_dev * cap // 16) * 16
    folded = tuple(c for c in late if widths[c] == 192 and tok_dev % 16 == 0)

    def room(*shape):
        rows = shape[-1]
        return [
            pltpu.VMEM(shape[:-1] + ((-(-rows * 3 // 32) * 16, 128) if c in folded else (rows, w)), BF16)
            for c, w in enumerate(widths)
        ]

    cfg = (ep, dp, tok_dev, chosen, experts, exp_dev, cap, packed, widths, starts, swapped, late, crossed, direct, held, folded, tok_dev * ep * dp)
    scratch = room(line, tok_dev) + room(line, packed) + room(line, packed) + room(ep, height)
    scratch += room(2, height) + room(height) + room(height) + room(height)
    scratch += [
        pltpu.VMEM((tok_dev, width), BF16),
        pltpu.VMEM((experts, width), BF16),
        pltpu.VMEM((1, experts), F32),
        pltpu.VMEM((1, 1), F32),
        dma((5,)),
        pltpu.VMEM((1, 1), F32),
        dma,
        pltpu.VMEM((tok_dev, 192), BF16),
        pltpu.VMEM((exp_dev, cap * ep, width), BF16),
        pltpu.VMEM((exp_dev, ep * (-(-cap // 8) * 8), max(widths)), F32),
        pltpu.VMEM((2, 8, tok_dev), F32),
        pltpu.VMEM((2, 8, tok_dev), F32),
        pltpu.VMEM((2, exp_dev, tok_dev), F32),
        pltpu.VMEM((dp, 2, exp_dev, tok_dev), F32),
        *[dma((max(len(swapped), 1),))] * 3, *[dma((max(len(crossed), 1),))] * 3, dma, dma,
        pltpu.VMEM((8, tok_dev), F32),
        pltpu.VMEM((8, tok_dev), F32),
        pltpu.VMEM((ep, chosen, tok_dev), jnp.int32),
        pltpu.VMEM((line, packed, tok_dev), BF16),
        pltpu.VMEM((line, packed, tok_dev), BF16),
        pltpu.VMEM((line, 8, tok_dev), F32),
        pltpu.VMEM((line, 8, packed), F32),
        pltpu.VMEM((line, 8, tok_dev), F32),
        pltpu.VMEM((line, 8, packed), F32),
        pltpu.VMEM((ep, exp_dev, tok_dev), F32),
        pltpu.VMEM((dp * ep, exp_dev, tok_dev), F32),
        pltpu.VMEM((dp, tok_dev, part), BF16),
        pltpu.VMEM((dp, tok_dev, part), BF16),
        pltpu.VMEM((dp, 2, experts, tok_dev), F32),
        pltpu.VMEM((dp, exp_dev, tok_dev), F32),
        pltpu.VMEM((dp, 8, experts), F32),
        pltpu.VMEM((ep, 8, experts), F32),
        pltpu.VMEM((dp, experts, tok_dev), BF16),
        pltpu.VMEM((ep, exp_dev, part), F32),
        pltpu.VMEM((ep, exp_dev, part), F32),
        dma, dma((chunks,)), dma((3,)), dma((ep,)),
        dma((chunks,)), dma((chunks,)), dma((max(line - 1, 1), chunks)),
        dma((chunks,)), dma((line, chunks)), dma, dma,
        dma, dma, dma, dma, dma, dma, pltpu.SemaphoreType.REGULAR((max(line - 1, 1),)),
        dma, dma, dma, dma, dma, dma,
    ]
    token_grad, wg, loss = pl.pallas_call(
        functools.partial(kernel, cfg),
        name="router_backward",
        out_shape=(
            pltpu.VMEM((tok_dev, width), BF16),
            pltpu.VMEM((exp_dev, part), F32),
            jax.ShapeDtypeStruct((1, 1), F32),
        ),
        in_specs=[hbm] * 7,
        out_specs=(vmem, vmem, hbm),
        scratch_shapes=scratch,
        compiler_params=pltpu.CompilerParams(
            collective_id=0, has_side_effects=True, vmem_limit_bytes=56 * 1024 * 1024
        ),
    )(indices.T, out_grad, rows_t, tokens, router_weight.T, router_bias.reshape(1, experts), balance_scale.reshape(1, 1))
    token_grad, wg = pl.pallas_call(
        finish,
        name="write_out",
        out_shape=(
            jax.ShapeDtypeStruct(token_grad.shape, token_grad.dtype),
            jax.ShapeDtypeStruct(wg.shape, wg.dtype),
        ),
        in_specs=[vmem, vmem],
        out_specs=(hbm, hbm),
        scratch_shapes=[dma((2,))],
    )(*(pltpu.with_memory_space_constraint(x, pltpu.VMEM) for x in (token_grad, wg)))
    return (token_grad, wg.T, loss.reshape(1))


def solution(mesh):
    placed = (
        P(("ep", "dp"), None),
        P(("ep", "dp"), None),
        P(("ep", "dp"), None),
        P("dp", "ep", None, None, None),
        P(),
        P(),
        P(),
    )
    return jax.shard_map(
        on_device,
        mesh=mesh,
        in_specs=placed,
        out_specs=(P(("ep", "dp"), None), P("dp", "ep"), P()),
        check_vma=False,
    )
```

```python
import functools
import math

import jax
import jax.numpy as jnp
from jax import lax
from jax.experimental import pallas as pl
from jax.experimental.pallas import tpu as pltpu
from jax.sharding import PartitionSpec as P

MESH = pl.DeviceIdType.MESH
F32 = jnp.float32
BF16 = jnp.bfloat16
CHUNK = 768
LAG = 4


def dot_nt(x, y, precision=None):
    return lax.dot_general(
        x, y, (((1,), (1,)), ((), ())), preferred_element_type=F32, precision=precision
    )


def dot_nn(x, y, precision=None):
    return lax.dot_general(
        x, y, (((1,), (0,)), ((), ())), preferred_element_type=F32, precision=precision
    )


def fold(left, right):
    half = right.shape[0] // 2
    pieces = [left, jnp.concatenate([right[0:half], right[half:]], axis=1)]
    short = -3 * half % 16
    if short:
        pieces.append(jnp.zeros((short, 128), F32))
    return jnp.concatenate(pieces, axis=0)


def unfold(x, rows):
    low = x[rows:, :].astype(F32)[0:rows // 2]
    return x[0:rows], jnp.concatenate([low[:, 0:64], low[:, 64:128]], axis=0).astype(BF16)


def kernel(cfg, *refs):
    (ep, dp, tok_dev, chosen, experts, exp_dev, cap, packed, widths, starts, swapped, late, crossed, direct, held, folded, token_total) = cfg
    line = ep // 2
    last = line - 1
    chunks = len(widths)
    every = range(chunks)
    kept = [c for c in every if c not in swapped]
    (idx_in, grad_in, rows_in, tok_in, wt_in, bias_in, scale_in, tg_out, wg_out, loss_out) = refs[:10]
    refs = refs[10:]
    hop = refs[5 * chunks:6 * chunks]
    hop_n = refs[6 * chunks:7 * chunks]
    back_n = refs[7 * chunks:8 * chunks]
    xb = refs[:chunks]
    lsend = refs[chunks:2 * chunks]
    lrecv = refs[2 * chunks:3 * chunks]
    rows_v = refs[3 * chunks:4 * chunks]
    back = refs[4 * chunks:5 * chunks]
    (tok_v, wt_v, bias_v, scale_v, s_in, loss_v, s_out, stage,
     rows_raw, piled, tgt_r, acc_r, rst_r, rbuf_r, s_back, r_back, r_hop, s_near, r_hop_n, r_back_n, s_rr, r_rr, tgt_n, acc_n,
     idx_all, pin, pout, tgt_x, tgt_p, acc_x, acc_p, rst, rbuf, tks, tkr, mp, nbuf, st_dp, st_ep, lgd, ws, wr,
     s_rows, s_own, s_idx, r_idx, s_right, s_left, r_x, s_leaf, r_leaf, s_rep, r_rep,
     s_tk, r_tk, s_sd, r_sd, s_se, r_se, s_ready, s_mp, r_mp, s_nb, r_nb, s_w, r_w) = refs[8 * chunks:]
    me = lax.axis_index("ep")
    md = lax.axis_index("dp")
    pos = me // 2
    side = lax.rem(me, 2)
    mate = pos * 2 + 1 - side
    at_end = jnp.logical_or(pos == 0, pos == last)
    near_end = jnp.logical_or(pos == 1, pos == last - 1)
    end = jnp.where(pos * 2 < line, 0, last)
    near = jnp.where(pos * 2 < line, 1, last - 1)
    far = last - end

    def ep_id(other):
        return (other, md)

    def remote(src, dst, s, r, dev):
        return pltpu.make_async_remote_copy(
            src_ref=src, dst_ref=dst, send_sem=s, recv_sem=r, device_id=dev, device_id_type=MESH
        )

    def ep_peer(s):
        return lax.rem(me + s, ep)

    def dp_peer(s):
        return lax.rem(md + s, dp)

    barrier = pltpu.get_barrier_semaphore()

    def greet(dev):
        pl.semaphore_signal(barrier, inc=1, device_id=dev, device_id_type=MESH)

    @pl.when(pos < last)
    def _():
        greet(ep_id(me + 2))

    @pl.when(pos > 0)
    def _():
        greet(ep_id(me - 2))

    greet(ep_id(mate))
    for s in range(1, dp):
        greet((me, dp_peer(s)))

    idx_here = pltpu.make_async_copy(idx_in, idx_all.at[me], s_in.at[0])
    own = [
        pltpu.make_async_copy(
            grad_in.at[:, pl.ds(starts[c], widths[c])], stage if c in folded else xb[c].at[pos], s_own.at[c]
        )
        for c in every
    ]
    rows_copy = pltpu.make_async_copy(rows_in, rows_raw, s_rows)
    small = [
        pltpu.make_async_copy(tok_in, tok_v, s_in.at[1]),
        pltpu.make_async_copy(wt_in, wt_v, s_in.at[2]),
        pltpu.make_async_copy(bias_in, bias_v, s_in.at[3]),
        pltpu.make_async_copy(scale_in, scale_v, s_in.at[4]),
    ]
    idx_here.start()
    for copy in own:
        copy.start()
    rows_copy.start()
    for copy in small:
        copy.start()
    pl.semaphore_wait(
        barrier, dp + (pos < last).astype(jnp.int32) + (pos > 0).astype(jnp.int32)
    )

    def idx_copy(q, way, dev):
        at = q * 2 + side
        return remote(idx_all.at[at], idx_all.at[at], s_idx.at[way], r_idx.at[at], ep_id(dev))

    def idx_right(q):
        return idx_copy(q, 0, me + 2)

    def idx_left(q):
        return idx_copy(q, 1, me - 2)

    def idx_mate(q):
        return idx_copy(q, 2, mate)

    def idx_from_mate(q):
        at = q * 2 + 1 - side
        return remote(idx_all.at[at], idx_all.at[at], s_idx.at[2], r_idx.at[at], ep_id(mate))

    def loop_ep(fn):
        def body(s, carry):
            fn(s)
            return carry
        lax.fori_loop(1, ep, body, 0)

    def to_right(q, c):
        return remote(xb[c].at[q], xb[c].at[q], s_right.at[c], r_x.at[q, c], ep_id(me + 2))

    def to_left(q, c):
        return remote(xb[c].at[q], xb[c].at[q], s_left.at[c], r_x.at[q - 1, c], ep_id(me - 2))

    def leaf(q, c):
        return remote(lsend[c].at[q], lrecv[c].at[q], s_leaf.at[c], r_leaf.at[q, c], ep_id(mate))

    def hop_rows(c):
        return remote(rows_v[c].at[far * 2 + 1 - side], hop[c], s_back.at[swapped.index(c)], r_hop.at[swapped.index(c)], ep_id(mate))

    def send_back(b, c):
        src = rows_v[c].at[far * 2 + side] if b == 0 else hop[c]
        at = side if b == 0 else 1 - side
        return remote(src, back[c].at[at], s_back.at[swapped.index(c)], r_back.at[swapped.index(c)], ep_id(near * 2 + side))

    def back_arrival(c):
        return remote(back[c], back[c], s_back.at[swapped.index(c)], r_back.at[swapped.index(c)], ep_id(end * 2 + side))

    def hop_near(c):
        n = crossed.index(c)
        return remote(rows_v[c].at[near * 2 + 1 - side], hop_n[c], s_near.at[n], r_hop_n.at[n], ep_id(mate))

    def send_near(c):
        n = crossed.index(c)
        if c in direct:
            return remote(rows_v[c].at[near * 2 + 1 - side], back_n[c], s_near.at[n], r_back_n.at[n], ep_id(near * 2 + 1 - side))
        return remote(hop_n[c], back_n[c], s_near.at[n], r_back_n.at[n], ep_id(near * 2 + side))

    def near_arrival(c):
        n = crossed.index(c)
        return remote(back_n[c], back_n[c], s_near.at[n], r_back_n.at[n], ep_id(end * 2 + side))

    def back_reply(d):
        return remote(rst_r, rbuf_r.at[md], s_rr, r_rr, (far * 2 + side, d))

    def back_replies():
        return remote(rbuf_r, rbuf_r, s_rr, r_rr, ep_id((last - near) * 2 + side))

    def reply(j, d):
        return remote(rst.at[j], rbuf.at[md * ep + me], s_rep, r_rep, (j, d))

    def replies():
        piece = rbuf.at[pl.ds(0, ep * dp - 1)]
        return remote(piece, piece, s_rep, r_rep, ep_id(mate))

    def near_share(s):
        return remote(nbuf.at[md], nbuf.at[md], s_nb, r_nb, (me, dp_peer(s)))

    def near_shares():
        piece = nbuf.at[pl.ds(0, dp - 1)]
        return remote(piece, piece, s_nb, r_nb, (me, dp_peer(1)))

    def mp_copy(s):
        return remote(mp.at[md], mp.at[md], s_mp, r_mp, (me, dp_peer(s)))

    def mp_all():
        piece = mp.at[pl.ds(0, dp - 1)]
        return remote(piece, piece, s_mp, r_mp, (me, dp_peer(1)))

    def se_copy(s):
        return remote(st_ep.at[me], st_ep.at[me], s_se, r_se, ep_id(ep_peer(s)))

    def se_all():
        return remote(st_ep.at[pl.ds(0, ep - 1)], st_ep.at[pl.ds(0, ep - 1)], s_se, r_se, ep_id(mate))

    def say_ready(n):
        def tell(dev):
            pl.semaphore_signal(s_ready.at[n], inc=1, device_id=ep_id(dev), device_id_type=MESH)

        @pl.when(pos < last)
        def _():
            tell(me + 2)

        @pl.when(pos > 0)
        def _():
            tell(me - 2)

        tell(mate)

    def hear_ready(n):
        pl.semaphore_wait(s_ready.at[n], 1 + (pos < last).astype(jnp.int32) + (pos > 0).astype(jnp.int32))
        if n + 1 < last:
            say_ready(n + 1)

    if last > 0:
        say_ready(0)
    for copy in own:
        copy.wait()
    idx_here.wait()

    @pl.when(pos < last)
    def _():
        idx_right(pos).start()

    @pl.when(pos > 0)
    def _():
        idx_left(pos).start()

    idx_mate(pos).start()
    for c in every:
        if c in folded:
            xb[c][pos] = fold(stage[:, 0:128].astype(F32), stage[:, 128:192].astype(F32)).astype(BF16)

        @pl.when(pos < last - (c in late))
        def _():
            to_right(pos, c).start()

        @pl.when(pos > 0 + (c in late))
        def _():
            to_left(pos, c).start()

    expert_row = lax.broadcasted_iota(jnp.int32, (experts, tok_dev), 0)
    eye_r = lax.broadcasted_iota(jnp.int32, (experts, experts), 0)
    eye_c = lax.broadcasted_iota(jnp.int32, (experts, experts), 1)
    t_from = lax.broadcasted_iota(jnp.int32, (tok_dev, tok_dev), 0)
    t_to = lax.broadcasted_iota(jnp.int32, (tok_dev, tok_dev), 1)
    upper = jnp.where(t_from < t_to, 1.0, 0.0).astype(BF16)
    row8 = lax.broadcasted_iota(jnp.int32, (8, tok_dev), 0)
    slot_p = lax.broadcasted_iota(jnp.int32, (packed, tok_dev), 0).astype(F32)

    def upright(line_of):
        return jnp.sum(jnp.where(eye_r == eye_c, line_of, 0.0), axis=1, keepdims=True)

    def plan(table, group):
        who = jnp.where(row8 < exp_dev, group * exp_dev + row8, -2)
        hit = jnp.zeros((8, tok_dev), F32)
        for k in range(chosen):
            hit = hit + jnp.where(table[k:k + 1, :] == who, 1.0, 0.0)
        need = jnp.max(hit, axis=0, keepdims=True)
        stack = jnp.where(row8 == exp_dev, need, hit)
        before = dot_nn(stack.astype(BF16), upper)
        place = jnp.where(need > 0.5, before[exp_dev:exp_dev + 1, :], -1.0)
        target = jnp.where(hit > 0.5, before, -1.0)
        pack = jnp.where(slot_p == place, 1.0, 0.0).astype(BF16)
        return target, pack

    def plan_block(q):
        table = idx_all[q * 2 + side]
        _, pack = plan(table, mate)
        pout[q] = pack
        target, _ = plan(table, me)
        tgt_x[q] = target
        acc_x[q] = jnp.zeros((8, tok_dev), F32)

    def plan_leaf(q):
        target, pack = plan(idx_all[q * 2 + 1 - side], me)
        pin[q] = pack
        tgt_p[q] = dot_nt((target + 1.0).astype(BF16), pack) - 1.0
        acc_p[q] = jnp.zeros((8, packed), F32)

    def plan_back():
        for b in range(2):
            tgt_r[b], _ = plan(idx_all[far * 2 + side], end * 2 + b)
            acc_r[b] = jnp.zeros((8, tok_dev), F32)
        tgt_n[...], _ = plan(idx_all[me], end * 2 + 1 - side)
        acc_n[...] = jnp.zeros((8, tok_dev), F32)

    deep = piled.shape[1] // ep
    slot_r = lax.broadcasted_iota(jnp.int32, (deep, cap * ep), 0)
    lies = lax.broadcasted_iota(jnp.int32, (deep, cap * ep), 1)
    spare = -exp_dev * cap % 16

    def sort_rows(c):
        w = widths[c]
        order = jnp.concatenate(
            [jnp.where(jnp.logical_and(lies == slot_r * ep + j, slot_r < cap), 1.0, 0.0) for j in range(ep)], axis=0
        ).astype(BF16)
        for e in range(exp_dev):
            piled[e, :, 0:w] = dot_nn(order, rows_raw[e, :, starts[c]:starts[c] + w])

        def put(j, carry):
            at = pl.ds(pl.multiple_of(j * deep, 8), deep)
            pieces = [piled[e, at, 0:w][0:cap, :] for e in range(exp_dev)]
            if spare:
                pieces.append(jnp.zeros((spare, w), F32))
            block = jnp.concatenate(pieces, axis=0)
            if c in folded:
                block = fold(block[:, 0:128], block[:, 128:192])
            rows_v[c][j] = block.astype(BF16)
            return carry

        lax.fori_loop(0, ep, put, 0)

    def all_dots(c, table, block, count):
        if c not in folded:
            return dot_nt(table, block)
        (table_l, table_r), (block_l, block_r) = unfold(table, exp_dev * cap + spare), unfold(block, count)
        return dot_nt(table_l, block_l) + dot_nt(table_r, block_r)

    def gathered(c, table, block, target, count):
        dots = all_dots(c, table, block, count)
        height = dots.shape[0]
        slot = lax.broadcasted_iota(jnp.int32, (height, count), 0).astype(F32)
        row = lax.broadcasted_iota(jnp.int32, (8, count), 0)
        out = jnp.zeros((8, count), F32)
        for e in range(exp_dev):
            want = jnp.where(target[e:e + 1, :] >= 0.0, target[e:e + 1, :] + e * cap, -1.0)
            one = jnp.sum(jnp.where(slot == want, dots, 0.0), axis=0, keepdims=True)
            out = jnp.where(row == e, one, out)
        return out

    def give_leaf(q, c):
        if c in folded:
            left, right = unfold(xb[c][q], tok_dev)
            lsend[c][q] = fold(dot_nn(pout[q], left), dot_nn(pout[q], right)).astype(BF16)
        else:
            lsend[c][q] = dot_nn(pout[q], xb[c][q]).astype(BF16)
        leaf(q, c).start()

    def use_block(q, c):
        acc_x[q] += gathered(c, rows_v[c][q * 2 + side], xb[c][q], tgt_x[q], tok_dev)

    def use_leaf(q, c):
        leaf(q, c).wait_recv()
        acc_p[q] += gathered(c, rows_v[c][q * 2 + 1 - side], lrecv[c][q], tgt_p[q], packed)

    def answer(j, value):
        rst[j] = value[0:exp_dev]
        for d in range(dp):
            reply(j, d).start()

    def done_block(q):
        answer(q * 2 + side, acc_x[q])

    def done_leaf(q):
        answer(q * 2 + 1 - side, dot_nn(acc_p[q], pin[q].astype(F32), lax.Precision.HIGHEST))

    def meets(s, c, tail):
        left, right = pos - s >= 0, pos + s < line
        if s == last and c in swapped:
            return ()
        if s == 1 and c in late:
            inner = at_end if tail else jnp.logical_not(at_end)
            left, right = jnp.logical_and(left, inner), jnp.logical_and(right, inner)
        return ((pos - s, left, True), (pos + s, right, False))

    def closes(s, c, tail, finish, q):
        if s == 1 and len(late):
            ends = [n for n in late if finish is done_block or n not in crossed]
            if tail:
                if c == ends[-1]:
                    finish(q)
            elif c == chunks - 1:
                @pl.when(jnp.logical_not(at_end))
                def _():
                    finish(q)
        elif c == (kept[-1] if s == last else chunks - 1):
            finish(q)

    def learn(s):
        for q, ok, rightward in ((pos - s, pos - s >= 0, True), (pos + s, pos + s < line, False)):
            @pl.when(ok)
            def _(q=q, rightward=rightward):
                step = idx_right if rightward else idx_left
                step(q).wait_recv()

                @pl.when(pos < last if rightward else pos > 0)
                def _():
                    step(q).start()
                    if s == last - 1 and len(swapped):
                        plan_back()

                idx_mate(q).start()
                plan_block(q)

    def learn_leaf(s):
        for q, ok in ((pos - s, pos - s >= 0), (pos + s, pos + s < line))[:1 if s == 0 else 2]:
            @pl.when(ok)
            def _(q=q):
                idx_from_mate(q).wait_recv()
                plan_leaf(q)

    def arrive(s, c, tail=False):
        for q, ok, rightward in meets(s, c, tail):
            @pl.when(ok)
            def _(q=q, rightward=rightward):
                step = to_right if rightward else to_left
                step(q, c).wait_recv()

                @pl.when(pos < last if rightward else pos > 0)
                def _():
                    if not (s == last - 1 and c in swapped):
                        step(q, c).start()
                    if s == last - 1 and c == kept[-1]:
                        for n in late:
                            step(pos, n).start()

                if not (tail and c in crossed):
                    give_leaf(q, c)
                if s == last - 1 and c == chunks - 1 and len(held):
                    @pl.when(pos < last if rightward else pos > 0)
                    def _():
                        for n in held:
                            give_leaf(pos, n)

    def use(s, c, tail=False):
        for q, ok, rightward in meets(s, c, tail):
            @pl.when(ok)
            def _(q=q, rightward=rightward):
                use_block(q, c)
                closes(s, c, tail, done_block, q)
                if s == last - 1 and len(swapped) and c == chunks - 1:
                    @pl.when(pos < last if rightward else pos > 0)
                    def _():
                        for m in swapped:
                            back_arrival(m).wait_recv()
                            for b in range(2):
                                acc_r[b] += gathered(m, back[m][b], xb[m][q], tgt_r[b], tok_dev)
                        rst_r[...] = acc_r[:, 0:exp_dev, :]
                        for d in range(dp):
                            back_reply(d).start()
                        for n in crossed:
                            near_arrival(n).wait_recv()
                            acc_n[...] += gathered(n, back_n[n][...], xb[n][pos], tgt_n[...], tok_dev)
                        nbuf[md] = acc_n[0:exp_dev]
                        for n in range(1, dp):
                            near_share(n).start()

    def take(s, c, tail=False):
        if s == 0:
            if len(held) and (c in held or c == chunks - 1):
                if c not in held:
                    use_leaf(pos, c)

                @pl.when(near_end if tail else jnp.logical_not(near_end))
                def _():
                    if c in held:
                        use_leaf(pos, c)
                    if c == (held[-1] if tail else chunks - 1):
                        done_leaf(pos)
            else:
                use_leaf(pos, c)
                if c == chunks - 1:
                    done_leaf(pos)
            return
        for q, ok, _ in meets(s, c, tail):
            @pl.when(ok)
            def _(q=q):
                use_leaf(q, c)
                closes(s, c, tail, done_leaf, q)

    def settle(s, c):
        if c == 0:
            learn_leaf(s)
        take(s, c)

    def pass_rows(c):
        @pl.when(at_end)
        def _():
            if c in swapped:
                hop_rows(c).wait_recv()
                send_back(1, c).start()
            if c in crossed and c not in direct:
                hop_near(c).wait_recv()
                send_near(c).start()

    def sort_step(c):
        sort_rows(c)
        if c in swapped or c in crossed:
            @pl.when(at_end)
            def _():
                if c in swapped:
                    hop_rows(c).start()
                    send_back(0, c).start()
                if c in direct:
                    send_near(c).start()
                elif c in crossed:
                    hop_near(c).start()
        use_block(pos, c)
        if c == chunks - 1:
            rst[me] = acc_x[pos][0:exp_dev]
            rbuf[md * ep + me] = acc_x[pos][0:exp_dev]
            for n in range(1, dp):
                reply(me, dp_peer(n)).start()

    part = tok_in.shape[1] // dp

    def tk_copy(s):
        return remote(tks.at[dp_peer(s)], tkr.at[md], s_tk, r_tk, (me, dp_peer(s)))

    def tk_all():
        return remote(tks.at[pl.ds(0, dp - 1)], tkr.at[pl.ds(0, dp - 1)], s_tk, r_tk, (me, dp_peer(1)))

    def sd_copy(s):
        return remote(st_dp.at[md], st_dp.at[md], s_sd, r_sd, (me, dp_peer(s)))

    def sd_all():
        return remote(st_dp.at[pl.ds(0, dp - 1)], st_dp.at[pl.ds(0, dp - 1)], s_sd, r_sd, (me, dp_peer(1)))

    def route():
        for copy in small:
            copy.wait()
        idx = idx_all[me]
        named = jnp.zeros((experts, tok_dev), F32)
        for k in range(chosen):
            named = named + jnp.where(idx[k:k + 1, :] == expert_row, 1.0, 0.0)
        logits = dot_nt(wt_v[...], tok_v[...]) + upright(bias_v[...])
        top = jnp.max(logits, axis=0, keepdims=True)
        power = jnp.exp(logits - top)
        prob = power / jnp.sum(power, axis=0, keepdims=True)
        high = jnp.max(jnp.where(named > 0.5, logits, -jnp.inf), axis=0, keepdims=True)
        mix = jnp.where(named > 0.5, jnp.exp(jnp.minimum(logits - high, 0.0)), 0.0)
        mp[md, 0] = mix / jnp.sum(mix, axis=0, keepdims=True)
        mp[md, 1] = prob
        ones = jnp.ones((8, tok_dev), F32)
        count_row = dot_nt(ones, named, lax.Precision.HIGHEST)
        prob_row = dot_nt(ones, prob, lax.Precision.HIGHEST)
        stat_row = lax.broadcasted_iota(jnp.int32, (8, experts), 0)
        st_dp[md] = jnp.where(stat_row == 0, count_row, prob_row)
        for s in range(1, dp):
            sd_copy(s).start()
        for s in range(1, dp):
            mp_copy(s).start()

    def share_tokens():
        for d in range(dp):
            tks[d] = tok_v[:, d * part:(d + 1) * part]
        for s in range(1, dp):
            tk_copy(s).start()
        tkr[md] = tks[md]

    def share_stats():
        sd_all().wait_recv()
        total = st_dp[0]
        for d in range(1, dp):
            total = total + st_dp[d]
        st_ep[me] = total
        loop_ep(lambda s: se_copy(s).start())

    plan_block(pos)
    for c in every:
        if c in held:
            @pl.when(jnp.logical_not(near_end))
            def _():
                give_leaf(pos, c)
        else:
            give_leaf(pos, c)
    rows_copy.wait()
    for c in every:
        if c == max(chunks - 2, 0):
            learn(1)
            arrive(1, 0)
        sort_step(c)
        if c < last:
            hear_ready(c)
    for n in range(chunks, last):
        hear_ready(n)
    steps = [(0, c) for c in every] + [(s, c) for s in range(1, line) for c in every]
    taken, tails = 0, []
    for n, (s, c) in enumerate(steps):
        if s == last and c in swapped:
            break
        if s > 0:
            if c == 0:
                if s > 1:
                    learn(s)
            if (s, c) != (1, 0):
                arrive(s, c)
            use(s, c)
            if s == 2:
                for n in every:
                    if (n in swapped or n in crossed) and c == (0 if n < 3 else n - 1):
                        pass_rows(n)
            if (s, c) == (1, 1 if chunks > 1 else 0):
                route()
                share_tokens()
            if (s, c) == (1, chunks - 1):
                share_stats()
            while taken <= n - LAG:
                settle(*steps[taken])
                taken += 1
    for m, c in enumerate(late):
        if m == 0 and taken < len(steps):
            settle(*steps[taken])
            taken += 1
        arrive(1, c, True)
        use(1, c, True)
        if m == 0:
            while taken < len(steps) and not (steps[taken][0] == last and steps[taken][1] in swapped):
                settle(*steps[taken])
                taken += 1
        if c not in crossed:
            tails.append(c)
    for step in steps[taken:]:
        settle(*step)
    for c in held:
        take(0, c, True)
    for c in tails:
        take(1, c, True)
    se_all().wait_recv()
    stats = lax.fori_loop(1, ep, lambda j, acc: acc + st_ep[j], st_ep[0])
    share = stats[0:1, :] / (token_total * chosen)
    mean = stats[1:2, :] / token_total
    loss_v[...] = experts * jnp.sum(share * mean, axis=1, keepdims=True)
    loss_copy = pltpu.make_async_copy(loss_v, loss_out, s_out)
    loss_copy.start()
    push_row = scale_v[...] * experts * share
    push = upright(push_row)
    mp_all().wait_recv()
    tk_all().wait_recv()
    spreads = []
    for d in range(dp):
        prob = mp[d, 1]
        spreads.append(prob * (push - jnp.sum(prob * push, axis=0, keepdims=True)))
    replies().wait_recv()
    if len(swapped):
        @pl.when(at_end)
        def _():
            back_replies().wait_recv()
            for d in range(dp):
                for b in range(2):
                    rbuf[d * ep + far * 2 + b] += rbuf_r[d, b]

        @pl.when(near_end)
        def _():
            near_shares().wait_recv()
            for d in range(dp):
                rbuf[d * ep + end * 2 + 1 - side] += nbuf[d]
    for d in range(dp):
        mix = mp[d, 0]
        dots = jnp.concatenate([rbuf[d * ep + j] for j in range(ep)], axis=0)
        sel = mix * (dots - jnp.sum(mix * dots, axis=0, keepdims=True))
        lgd[d] = (spreads[d] + sel).astype(BF16)
    term = dot_nn(lgd[0], tkr[0])
    for d in range(1, dp):
        term = term + dot_nn(lgd[d], tkr[d])
    for j in range(ep):
        ws[j] = term[j * exp_dev:(j + 1) * exp_dev, :]
    wr[me] = ws[me]

    def w_copy(s_):
        return remote(ws.at[ep_peer(s_)], wr.at[me], s_w, r_w, ep_id(ep_peer(s_)))

    def w_all():
        return remote(ws.at[pl.ds(0, ep - 1)], wr.at[pl.ds(0, ep - 1)], s_w, r_w, ep_id(mate))

    loop_ep(lambda s_: w_copy(s_).start())
    grad = lgd[md]
    for c in every:
        at = slice(starts[c], starts[c] + widths[c])
        tg_out[:, at] = lax.dot_general(
            grad, wt_v[:, at], (((0,), (0,)), ((), ())), preferred_element_type=F32
        ).astype(BF16)

    def sent(ref, sem, count):
        for n in range(1, line + 1):
            @pl.when(count == n)
            def _(n=n):
                piece = ref.at[pl.ds(0, n)]
                remote(piece, piece, sem, sem, ep_id(mate)).wait_send()

    ups = jnp.where(pos < last, pos + 1, 0)
    downs = jnp.where(pos > 0, line - pos, 0)
    sent(idx_all, s_idx.at[0], ups)
    sent(idx_all, s_idx.at[1], downs)
    sent(idx_all, s_idx.at[2], line)
    se_all().wait_send()
    for c in every:
        short = 1 if c in swapped else 0
        sent(xb[c], s_right.at[c], ups - jnp.where(pos == last - 1, short, 0))
        sent(xb[c], s_left.at[c], downs - jnp.where(pos == 1, short, 0))
        skipped = short + (1 if c in crossed else 0)
        sent(lsend[c], s_leaf.at[c], line - jnp.where(at_end, skipped, 0))
    if len(swapped):
        @pl.when(at_end)
        def _():
            for c in swapped:
                piece = rows_v[c].at[pl.ds(0, 3)]
                sem = s_back.at[swapped.index(c)]
                remote(piece, piece, sem, sem, ep_id(mate)).wait_send()
            for n, c in enumerate(crossed):
                piece = rows_v[c].at[pl.ds(0, 1 if c in direct else 2)]
                remote(piece, piece, s_near.at[n], s_near.at[n], ep_id(mate)).wait_send()

        @pl.when(near_end)
        def _():
            back_replies().wait_send()
            near_shares().wait_send()
    replies().wait_send()
    mp_all().wait_send()
    sd_all().wait_send()
    tk_all().wait_send()
    loss_copy.wait()
    w_all().wait_recv()
    out = lax.fori_loop(1, ep, lambda j, acc: acc + wr[j], wr[0])
    wg_out[...] = out / math.sqrt(token_total)
    w_all().wait_send()


def finish(tg_in, wg_in, tg_out, wg_out, sems):
    copies = [pltpu.make_async_copy(tg_in, tg_out, sems.at[0]), pltpu.make_async_copy(wg_in, wg_out, sems.at[1])]
    for copy in copies:
        copy.start()
    for copy in copies:
        copy.wait()


def cut(width):
    if width <= 3 * CHUNK + CHUNK // 2 or width > 4 * CHUNK:
        widths = tuple(min(CHUNK, width - s) for s in range(0, width, CHUNK))
        return widths, tuple(sum(widths[:c]) for c in range(len(widths))), (), (), (), (), ()
    half = CHUNK // 2
    rest = width - 3 * CHUNK - half
    return (CHUNK, rest, half, CHUNK, CHUNK), (0, width - rest, CHUNK, CHUNK + half, 2 * CHUNK + half), (2, 3, 4), (4, 2, 1), (2, 1), (2,), (4,)


def on_device(tokens, out_grad, indices, expert_rows, router_weight, router_bias, balance_scale):
    tok_dev, width = tokens.shape
    chosen = indices.shape[1]
    experts = router_weight.shape[1]
    exp_dev, cap = expert_rows.shape[1], expert_rows.shape[3]
    ep = lax.axis_size("ep")
    dp = lax.axis_size("dp")
    line = ep // 2
    packed = -(-min(tok_dev, (exp_dev - 1) * cap) // 16) * 16
    widths, starts, swapped, late, crossed, direct, held = cut(width)
    chunks = len(widths)
    if line < 4:
        swapped, late, crossed, direct, held = (), (), (), (), ()
    part = width // dp
    rows_t = jnp.transpose(expert_rows[0], (0, 2, 1, 3)).reshape(exp_dev, cap * ep, width)
    hbm = pl.BlockSpec(memory_space=pl.ANY)
    vmem = pl.BlockSpec(memory_space=pltpu.VMEM)
    dma = pltpu.SemaphoreType.DMA
    height = -(-exp_dev * cap // 16) * 16
    folded = tuple(c for c in late if widths[c] == 192 and tok_dev % 16 == 0)

    def room(*shape):
        rows = shape[-1]
        return [
            pltpu.VMEM(shape[:-1] + ((-(-rows * 3 // 32) * 16, 128) if c in folded else (rows, w)), BF16)
            for c, w in enumerate(widths)
        ]

    cfg = (ep, dp, tok_dev, chosen, experts, exp_dev, cap, packed, widths, starts, swapped, late, crossed, direct, held, folded, tok_dev * ep * dp)
    scratch = room(line, tok_dev) + room(line, packed) + room(line, packed) + room(ep, height)
    scratch += room(2, height) + room(height) + room(height) + room(height)
    scratch += [
        pltpu.VMEM((tok_dev, width), BF16),
        pltpu.VMEM((experts, width), BF16),
        pltpu.VMEM((1, experts), F32),
        pltpu.VMEM((1, 1), F32),
        dma((5,)),
        pltpu.VMEM((1, 1), F32),
        dma,
        pltpu.VMEM((tok_dev, 192), BF16),
        pltpu.VMEM((exp_dev, cap * ep, width), BF16),
        pltpu.VMEM((exp_dev, ep * (-(-cap // 8) * 8), max(widths)), F32),
        pltpu.VMEM((2, 8, tok_dev), F32),
        pltpu.VMEM((2, 8, tok_dev), F32),
        pltpu.VMEM((2, exp_dev, tok_dev), F32),
        pltpu.VMEM((dp, 2, exp_dev, tok_dev), F32),
        *[dma((max(len(swapped), 1),))] * 3, *[dma((max(len(crossed), 1),))] * 3, dma, dma,
        pltpu.VMEM((8, tok_dev), F32),
        pltpu.VMEM((8, tok_dev), F32),
        pltpu.VMEM((ep, chosen, tok_dev), jnp.int32),
        pltpu.VMEM((line, packed, tok_dev), BF16),
        pltpu.VMEM((line, packed, tok_dev), BF16),
        pltpu.VMEM((line, 8, tok_dev), F32),
        pltpu.VMEM((line, 8, packed), F32),
        pltpu.VMEM((line, 8, tok_dev), F32),
        pltpu.VMEM((line, 8, packed), F32),
        pltpu.VMEM((ep, exp_dev, tok_dev), F32),
        pltpu.VMEM((dp * ep, exp_dev, tok_dev), F32),
        pltpu.VMEM((dp, tok_dev, part), BF16),
        pltpu.VMEM((dp, tok_dev, part), BF16),
        pltpu.VMEM((dp, 2, experts, tok_dev), F32),
        pltpu.VMEM((dp, exp_dev, tok_dev), F32),
        pltpu.VMEM((dp, 8, experts), F32),
        pltpu.VMEM((ep, 8, experts), F32),
        pltpu.VMEM((dp, experts, tok_dev), BF16),
        pltpu.VMEM((ep, exp_dev, part), F32),
        pltpu.VMEM((ep, exp_dev, part), F32),
        dma, dma((chunks,)), dma((3,)), dma((ep,)),
        dma((chunks,)), dma((chunks,)), dma((max(line - 1, 1), chunks)),
        dma((chunks,)), dma((line, chunks)), dma, dma,
        dma, dma, dma, dma, dma, dma, pltpu.SemaphoreType.REGULAR((max(line - 1, 1),)),
        dma, dma, dma, dma, dma, dma,
    ]
    token_grad, wg, loss = pl.pallas_call(
        functools.partial(kernel, cfg),
        name="router_backward",
        out_shape=(
            pltpu.VMEM((tok_dev, width), BF16),
            pltpu.VMEM((exp_dev, part), F32),
            jax.ShapeDtypeStruct((1, 1), F32),
        ),
        in_specs=[hbm] * 7,
        out_specs=(vmem, vmem, hbm),
        scratch_shapes=scratch,
        compiler_params=pltpu.CompilerParams(
            collective_id=0, has_side_effects=True, vmem_limit_bytes=56 * 1024 * 1024
        ),
    )(indices.T, out_grad, rows_t, tokens, router_weight.T, router_bias.reshape(1, experts), balance_scale.reshape(1, 1))
    token_grad, wg = pl.pallas_call(
        finish,
        name="write_out",
        out_shape=(
            jax.ShapeDtypeStruct(token_grad.shape, token_grad.dtype),
            jax.ShapeDtypeStruct(wg.shape, wg.dtype),
        ),
        in_specs=[vmem, vmem],
        out_specs=(hbm, hbm),
        scratch_shapes=[dma((2,))],
    )(*(pltpu.with_memory_space_constraint(x, pltpu.VMEM) for x in (token_grad, wg)))
    return (token_grad, wg.T, loss.reshape(1))


def solution(mesh):
    placed = (
        P(("ep", "dp"), None),
        P(("ep", "dp"), None),
        P(("ep", "dp"), None),
        P("dp", "ep", None, None, None),
        P(),
        P(),
        P(),
    )
    return jax.shard_map(
        on_device,
        mesh=mesh,
        in_specs=placed,
        out_specs=(P(("ep", "dp"), None), P("dp", "ep"), P()),
        check_vma=False,
    )
```
